8 devices in a mesh: dp: 1 (over z), tp: 8 (over x, y, core).
Axes of the slice: x: 2, y: 2, z: 1, core: 2. Of those that a mesh axis runs over, the one named last changes fastest.
Arguments:
- x: bfloat16 [1, 4096, 2048], P('dp', 'tp')
- dy: bfloat16 [1, 4096, 2048], P('dp', 'tp')
- wq: bfloat16 [2048, 2048], P(None, 'tp')
- wk: bfloat16 [2048, 2048], P(None, 'tp')
- wv: bfloat16 [2048, 2048], P(None, 'tp')
- wo: bfloat16 [2048, 2048], P('tp')
- w_gate: bfloat16 [2048, 8192], P(None, 'tp')
- w_up: bfloat16 [2048, 8192], P(None, 'tp')
- w_down: bfloat16 [8192, 2048], P('tp')
Outputs:
- output 1: bfloat16 [1, 4096, 2048], P('dp', 'tp')
- output 2: bfloat16 [2048, 2048], P('dp', 'tp')
- output 3: bfloat16 [2048, 2048], P('dp', 'tp')
- output 4: bfloat16 [2048, 2048], P('dp', 'tp')
- output 5: bfloat16 [2048, 2048], P(('dp', 'tp'))
- output 6: bfloat16 [2048, 8192], P('dp', 'tp')
- output 7: bfloat16 [2048, 8192], P('dp', 'tp')
- output 8: bfloat16 [8192, 2048], P(('dp', 'tp'))
All inputs are finite; a program needn't handle non-finite values.
Results may differ from the reference program's by a relative error of at most 0.024.
Values are sent between devices in bfloat16 or wider.
A program may use at most 2 GiB of HBM per device.

```python
import jax
import jax.numpy as jnp
from jax import lax

SEQUENCES = 1
TOKENS = 4096
D = 2048
HEADS = 16
KV_HEADS = 16
HEAD = 128
FF = 8192
THETA = 10000
NAMES = ("wq", "wk", "wv", "wo", "w_gate", "w_up", "w_down")
SHAPES = {
    "wq": (D, HEADS * HEAD),
    "wk": (D, KV_HEADS * HEAD),
    "wv": (D, KV_HEADS * HEAD),
    "wo": (HEADS * HEAD, D),
    "w_gate": (D, FF),
    "w_up": (D, FF),
    "w_down": (FF, D),
}


def bump(key, n, height):
    away = (jnp.arange(n, dtype=jnp.int32) - jax.random.randint(key, (), 0, n, jnp.int32)) % n
    return jnp.where(away < n // 8, height, 1.0)


def together(key, own, strength):
    shared = jax.random.normal(key, own.shape[1:], jnp.float32)
    return (own + strength * shared) * lax.rsqrt(1 + strength * strength)


def setup_inputs(seed: int = 0, part: int = 0) -> dict:
    kx, kdy, ka, kb, kz, kf, kh, kl, *kw = jax.random.split(jax.random.key(seed), 8 + len(NAMES))
    kx, kdy, ka, kb = (jax.random.fold_in(k, part) for k in (kx, kdy, ka, kb))
    shape = (SEQUENCES, TOKENS, D)
    much_x, much_dy = jax.random.uniform(kz, (2,), jnp.float32, 0.0, 1.0)
    loud = 2.0 ** jax.random.uniform(jax.random.fold_in(kz, 1), (), jnp.float32, -1.0, 2.0)
    halves = 2.0 ** jax.random.uniform(kl, (2,), jnp.float32, -1.0, 1.0)
    times = {"wq": 1.0, "wk": 1.0, "wv": 2.0, "wo": halves[0], "w_gate": 1.0, "w_up": bump(kh, FF, 4.0), "w_down": halves[1]}
    x = together(ka, jax.random.normal(kx, shape, jnp.float32), much_x) * bump(kf, D, 4.0)
    dy = together(kb, jax.random.normal(kdy, shape, jnp.float32), much_dy)
    drawn = {"x": x.astype(jnp.bfloat16), "dy": (loud * dy * (SEQUENCES * TOKENS) ** -0.5).astype(jnp.bfloat16)}
    for key, name in zip(kw, NAMES, strict=True):
        drawn[name] = (jax.random.normal(key, SHAPES[name], jnp.float32) * SHAPES[name][0] ** -0.5 * times[name]).astype(jnp.bfloat16)
    return drawn


def matmul(a, w):
    return jnp.dot(a, w, preferred_element_type=jnp.float32).astype(jnp.bfloat16)


def normed(h):
    wide = h.astype(jnp.float32)
    scale = lax.rsqrt(jnp.mean(wide**2, -1, keepdims=True) + 1e-6)
    return (wide * scale).astype(jnp.bfloat16)


def turned(t, theta):
    half = t.shape[-1] // 2
    angle = jnp.arange(t.shape[0], dtype=jnp.float32)[:, None] * theta ** (-jnp.arange(half, dtype=jnp.float32) / half)
    cos, sin = jnp.cos(angle)[:, None], jnp.sin(angle)[:, None]
    a, b = t[..., :half].astype(jnp.float32), t[..., half:].astype(jnp.float32)
    return jnp.concatenate([a * cos - b * sin, b * cos + a * sin], -1).astype(jnp.bfloat16)


def seen_by(q, k, v):
    tokens, kv = q.shape[0], k.shape[1]
    q = q.reshape(tokens, kv, -1, q.shape[-1])
    scores = jnp.einsum("tgsd,ugd->gstu", q.astype(jnp.float32), k.astype(jnp.float32)) * q.shape[-1] ** -0.5
    place = jnp.arange(tokens)
    weights = jax.nn.softmax(jnp.where(place[:, None] >= place, scores, -jnp.inf), -1).astype(jnp.bfloat16)
    return jnp.einsum("gstu,ugd->tgsd", weights.astype(jnp.float32), v.astype(jnp.float32)).astype(jnp.bfloat16).reshape(tokens, -1)


def layer(h, w):
    a = normed(h)
    q, k = (turned(matmul(a, w[name]).reshape(h.shape[0], -1, HEAD), THETA) for name in ("wq", "wk"))
    h = h + matmul(seen_by(q, k, matmul(a, w["wv"]).reshape(h.shape[0], -1, HEAD)), w["wo"])
    b = normed(h)
    gate = jnp.dot(b, w["w_gate"], preferred_element_type=jnp.float32)
    up = jnp.dot(b, w["w_up"], preferred_element_type=jnp.float32)
    return h + matmul((jax.nn.silu(gate) * up).astype(jnp.bfloat16), w["w_down"])


def reference(x, dy, wq, wk, wv, wo, w_gate, w_up, w_down):
    weights = dict(zip(NAMES, (wq, wk, wv, wo, w_gate, w_up, w_down), strict=True))

    def take(so_far, sequence):
        h, by_y = sequence
        _, back = jax.vjp(lambda w, h: layer(h, w), weights, h)
        by_weights, by_h = back(by_y)
        return jax.tree.map(lambda total, term: total + term.astype(jnp.float32), so_far, by_weights), by_h

    none_yet = {name: jnp.zeros(w.shape, jnp.float32) for name, w in weights.items()}
    by_weights, by_x = lax.scan(take, none_yet, (x, dy))
    return (by_x, *(by_weights[name].astype(jnp.bfloat16) for name in NAMES))
```

```python
import functools

import jax
import jax.numpy as jnp
from jax import lax
from jax.experimental import pallas as pl
from jax.experimental.pallas import tpu as pltpu
from jax.sharding import PartitionSpec as P


HEAD = 128
THETA = 10000
NEG = -1e30
HIDDEN = 2 * NEG
LOG2E = 1.4426950408889634
MIB = 2**20
VMEM = 60 * MIB
BF = jnp.bfloat16
F32 = jnp.float32
TP = 8


def _dot(a, b, ca=1, cb=0):
    return lax.dot_general(a, b, (((ca,), (cb,)), ((), ())), preferred_element_type=F32)


def _params(*semantics, vmem=VMEM):
    return pltpu.CompilerParams(dimension_semantics=semantics, vmem_limit_bytes=vmem)


def _cost(flops, *arrays):
    return pl.CostEstimate(flops=int(flops), transcendentals=0, bytes_accessed=int(sum(a.size * a.dtype.itemsize for a in arrays)))


def _like(shape, dtype=BF):
    return jax.ShapeDtypeStruct(shape, dtype)


def _scale_of(wide):
    return lax.rsqrt(jnp.mean(wide * wide, -1, keepdims=True) + 1e-6)


def _norm_body(x_ref, a_ref):
    wide = x_ref[...].astype(F32)
    a_ref[...] = (wide * _scale_of(wide)).astype(BF)


def norm(x):
    t, d = x.shape
    rows = 128
    spec = pl.BlockSpec((rows, d), lambda i: (i, 0))
    return pl.pallas_call(_norm_body, grid=(t // rows,), in_specs=[spec], out_specs=spec, out_shape=_like(x.shape), name="norm",
                          compiler_params=_params("arbitrary"), cost_estimate=_cost(2e9, x, x))(x)


def _norm_bwd_body(n, h_ref, base_ref, *rest):
    out_ref = rest[n]
    g = rest[0][...].astype(F32)
    for r in rest[1:n]:
        g = g + r[...].astype(F32)
    wide = h_ref[...].astype(F32)
    scale = _scale_of(wide)
    along = jnp.mean(g * wide, -1, keepdims=True)
    out_ref[...] = (base_ref[...].astype(F32) + scale * (g - wide * (scale * scale * along))).astype(BF)


def norm_bwd(h, base, terms):
    t, d = h.shape
    rows = 128
    spec = pl.BlockSpec((rows, d), lambda i: (i, 0))
    return pl.pallas_call(functools.partial(_norm_bwd_body, len(terms)), grid=(t // rows,), in_specs=[spec] * (2 + len(terms)), out_specs=spec,
                          out_shape=_like(h.shape), name="norm_bwd", compiler_params=_params("arbitrary"),
                          cost_estimate=_cost(2e9, h, base, *terms))(h, base, *terms)


def _turn(x, cos, sin):
    parts = [x[:, n : n + HEAD] for n in range(0, x.shape[1], HEAD)]
    return jnp.concatenate([p * cos + pltpu.roll(p, HEAD // 2, 1) * sin for p in parts], axis=1)


def _qkv_body(at_ref, a_ref, wq_ref, wk_ref, wv_ref, cos_ref, sin_ref, *rest):
    q_ref, k_ref, v_ref = rest[-3:]
    a = a_ref[...]
    cos, sin = cos_ref[...], sin_ref[...]
    q_ref[...] = _turn(_dot(a, wq_ref[...]).astype(BF).astype(F32), cos, sin).astype(BF)
    k_ref[...] = _turn(_dot(a, wk_ref[...]).astype(BF).astype(F32), cos, sin).astype(BF)
    v_ref[...] = _dot(a, wv_ref[...]).astype(BF)


def qkv(at, a, wq, wk, wv, cos, sin, before):
    t, d = a.shape
    n = wq.shape[1]
    rows = 256
    per = t // rows
    total = cos.shape[0]
    whole = pl.BlockSpec((d, n), lambda i, at: (0, 0))
    place = lambda i, at: (at[0] * per + i, 0)
    table = pl.BlockSpec((rows, HEAD), place)
    out = pl.BlockSpec((rows, n), place)
    grid_spec = pltpu.PrefetchScalarGridSpec(
        num_scalar_prefetch=1, grid=(per,),
        in_specs=[pl.BlockSpec((rows, d), lambda i, at: (i, 0)), whole, whole, whole, table, table] + [pl.BlockSpec(memory_space=pl.ANY)] * len(before),
        out_specs=[out] * 3)
    return pl.pallas_call(_qkv_body, grid_spec=grid_spec, out_shape=[_like((total, n))] * 3, name="qkv",
                          input_output_aliases={7 + n: n for n in range(len(before))}, compiler_params=_params("arbitrary"),
                          cost_estimate=_cost(6 * t * d * n, a, wq, wk, wv))(at, a, wq, wk, wv, cos, sin, *before)


def _diagonal(size):
    return lax.broadcasted_iota(jnp.int32, (size, size), 1) >= lax.broadcasted_iota(jnp.int32, (size, size), 0)


def _attend_body(q_ref, k_ref, v_ref, o_ref, lse_ref, top_s, mix_s, *, scale, b):
    bq, width = q_ref.shape
    heads, strips = width // HEAD, bq // b
    iq = pl.program_id(0)
    e = scale * LOG2E
    top_s[...] = jnp.full_like(top_s, NEG)
    mix_s[...] = jnp.zeros_like(mix_s)
    ones = jnp.ones((8, b), BF)

    def block(j, first):
        here = pl.ds(j * b, b)
        pieces = [(i, n) for i in range(heads) for n in range(first or 0, strips)]
        scores = [_dot(k_ref[here, i * HEAD : (i + 1) * HEAD], q_ref[n * b : (n + 1) * b, i * HEAD : (i + 1) * HEAD], 1, 1) for i, n in pieces]
        weights, keeps = [], []
        for (i, n), s in zip(pieces, scores):
            if n == first:
                s = jnp.where(_diagonal(b), s, HIDDEN)
            at = slice(n * b, (n + 1) * b)
            old = top_s[i : i + 1, at]
            top = jnp.maximum(old, s.max(axis=0, keepdims=True))
            top_s[i : i + 1, at] = top
            weights.append(jnp.exp2((s - top) * e).astype(BF))
            keeps.append(jnp.exp2((old - top) * e))
        for (i, n), p, keep in zip(pieces, weights, keeps):
            at = slice(n * b, (n + 1) * b)
            values = jnp.concatenate([v_ref[here, i * HEAD : (i + 1) * HEAD].T, ones], axis=0)
            mix_s[i, :, at] = mix_s[i, :, at] * keep + _dot(values, p)

    lax.fori_loop(0, iq * strips, lambda j, _: block(j, None), None)
    for n in range(strips):
        block(iq * strips + n, n)
    for i in range(heads):
        total = mix_s[i, HEAD : HEAD + 1, :]
        o_ref[:, i * HEAD : (i + 1) * HEAD] = (mix_s[i, :HEAD, :] * (1 / total)).T.astype(BF)
        lse_ref[i : i + 1, :] = top_s[i : i + 1, :] * scale + jnp.log(total)


def attend(q, k, v, bq=2048, b=512):
    t, n = q.shape
    heads = n // HEAD
    whole = pl.BlockSpec((t, n), lambda i: (0, 0))
    rows = pl.BlockSpec((bq, n), lambda i: (i, 0))
    return pl.pallas_call(
        functools.partial(_attend_body, scale=HEAD**-0.5, b=b), grid=(t // bq,), in_specs=[rows, whole, whole],
        out_specs=[rows, pl.BlockSpec((heads, bq), lambda i: (0, i))], out_shape=[_like((t, n)), _like((heads, t), F32)],
        scratch_shapes=[pltpu.VMEM((heads, bq), F32), pltpu.VMEM((heads, HEAD + 8, bq), F32)], name="attend",
        compiler_params=_params("arbitrary"), cost_estimate=_cost(4 * t * t * n, q, k, v, q))(q, k, v)


def _attend_bwd_body(q_ref, k_ref, v_ref, do_ref, o_ref, lse_ref, cosq_ref, sinq_ref, cos_ref, sin_ref, dq_ref, dk_ref, dv_ref, dq_s, dk_s, dv_s,
                     *, scale, b):
    bq, width = q_ref.shape
    heads, strips = width // HEAD, bq // b
    iq = pl.program_id(0)
    e = scale * LOG2E

    @pl.when(iq == 0)
    def _():
        dk_s[...] = jnp.zeros_like(dk_s)
        dv_s[...] = jnp.zeros_like(dv_s)

    dq_s[...] = jnp.zeros_like(dq_s)
    lses = [lse_ref[i : i + 1, :] * LOG2E for i in range(heads)]
    deltas = []
    for i in range(heads):
        at = slice(i * HEAD, (i + 1) * HEAD)
        deltas.append((do_ref[:, at].astype(F32) * o_ref[:, at].astype(F32)).T.sum(axis=0, keepdims=True))

    def block(j, first):
        here = pl.ds(j * b, b)
        pieces = [(i, n) for i in range(heads) for n in range(first or 0, strips)]
        qs = [q_ref[n * b : (n + 1) * b, i * HEAD : (i + 1) * HEAD] for i, n in pieces]
        dos = [do_ref[n * b : (n + 1) * b, i * HEAD : (i + 1) * HEAD] for i, n in pieces]
        scores = [_dot(k_ref[here, i * HEAD : (i + 1) * HEAD], x, 1, 1) for (i, _), x in zip(pieces, qs)]
        dps = [_dot(v_ref[here, i * HEAD : (i + 1) * HEAD], x, 1, 1) for (i, _), x in zip(pieces, dos)]
        for m, (i, n) in enumerate(pieces):
            at, head = slice(n * b, (n + 1) * b), slice(i * HEAD, (i + 1) * HEAD)
            p = jnp.exp2(scores[m] * e - lses[i][:, at])
            if n == first:
                p = jnp.where(_diagonal(b), p, 0.0)
            ds = (p * (dps[m] - deltas[i][:, at])).astype(BF)
            dv_s[here, head] += _dot(p.astype(BF), dos[m])
            dk_s[here, head] += _dot(ds, qs[m])
            dq_s[i, :, at] += _dot(k_ref[here, head].T, ds)

    lax.fori_loop(0, iq * strips, lambda j, _: block(j, None), None)
    for n in range(strips):
        block(iq * strips + n, n)

    def back(g, cos, sin):
        return _turn(g.astype(BF).astype(F32), cos, -sin).astype(BF)

    for i in range(heads):
        head = slice(i * HEAD, (i + 1) * HEAD)
        dq_ref[:, head] = back((dq_s[i] * scale).T, cosq_ref[...], sinq_ref[...])

    @pl.when(iq == pl.num_programs(0) - 1)
    def _():
        for i in range(heads):
            head = slice(i * HEAD, (i + 1) * HEAD)
            for r in range(0, dk_s.shape[0], b):
                rows = slice(r, r + b)
                dk_ref[rows, head] = back(dk_s[rows, head] * scale, cos_ref[rows, :], sin_ref[rows, :])
                dv_ref[rows, head] = dv_s[rows, head].astype(BF)


def attend_bwd(q, k, v, do, o, lse, cos, sin, bq=1024, b=512):
    t, n = q.shape
    heads = n // HEAD
    whole = pl.BlockSpec((t, n), lambda i: (0, 0))
    rows = pl.BlockSpec((bq, n), lambda i: (i, 0))
    part = pl.BlockSpec((bq, HEAD), lambda i: (i, 0))
    table = pl.BlockSpec((t, HEAD), lambda i: (0, 0))
    return pl.pallas_call(
        functools.partial(_attend_bwd_body, scale=HEAD**-0.5, b=b), grid=(t // bq,),
        in_specs=[rows, whole, whole, rows, rows, pl.BlockSpec((heads, bq), lambda i: (0, i)), part, part, table, table],
        out_specs=[rows, whole, whole], out_shape=[_like((t, n))] * 3,
        scratch_shapes=[pltpu.VMEM((heads, HEAD, bq), F32), pltpu.VMEM((t, n), F32), pltpu.VMEM((t, n), F32)], name="attend_bwd",
        compiler_params=_params("arbitrary"), cost_estimate=_cost(10 * t * t * n, q, k, v, do, o))(q, k, v, do, o, lse, cos, sin, cos, sin)


def _out_body(*refs):
    os, ws, (x_ref, h_ref, b_ref) = refs[:TP], refs[TP : 2 * TP], refs[2 * TP :]
    total = _dot(os[0][...], ws[0][...])
    for o_ref, w_ref in zip(os[1:], ws[1:]):
        total = total + _dot(o_ref[...], w_ref[...])
    h = (x_ref[...].astype(F32) + total.astype(BF).astype(F32)).astype(BF)
    h_ref[...] = h
    wide = h.astype(F32)
    b_ref[...] = (wide * _scale_of(wide)).astype(BF)


def out_proj(os, ws, x):
    t, d = x.shape
    n = os[0].shape[1]
    rows = 128
    own = pl.BlockSpec((rows, d), lambda i: (i, 0))
    return pl.pallas_call(
        _out_body, grid=(t // rows,),
        in_specs=[pl.BlockSpec((rows, n), lambda i: (i, 0))] * TP + [pl.BlockSpec((n, d), lambda i: (0, 0))] * TP + [own],
        out_specs=[own, own], out_shape=[_like((t, d))] * 2, name="out_proj", compiler_params=_params("arbitrary"),
        cost_estimate=_cost(2 * t * d * n * TP, *os, *ws, x))(*os, *ws, x)


def _out_bwd_body(g_ref, *refs):
    g = g_ref[...]
    for w_ref, o_ref in zip(refs[:TP], refs[TP:]):
        o_ref[...] = _dot(g, w_ref[...], 1, 1).astype(BF)


def out_proj_bwd(g, ws):
    t, d = g.shape
    n = ws[0].shape[0]
    rows = 256
    return pl.pallas_call(
        _out_bwd_body, grid=(t // rows,), in_specs=[pl.BlockSpec((rows, d), lambda i: (i, 0))] + [pl.BlockSpec((n, d), lambda i: (0, 0))] * TP,
        out_specs=[pl.BlockSpec((rows, n), lambda i: (i, 0))] * TP, out_shape=[_like((t, n))] * TP, name="out_proj_bwd",
        compiler_params=_params("arbitrary"), cost_estimate=_cost(2 * t * d * n * TP, g, *ws))(g, *ws)


def _hidden_body(b_ref, y_ref, wg_ref, wu_ref, wd_ref, hid_ref, dg_ref, du_ref):
    b = b_ref[...]
    gate, up = _dot(b, wg_ref[...]), _dot(b, wu_ref[...])
    g = _dot(y_ref[...], wd_ref[...], 1, 1).astype(BF).astype(F32)
    sig = 1 / (1 + jnp.exp(-gate))
    silu = gate * sig
    hid_ref[...] = (silu * up).astype(BF)
    du_ref[...] = (g * silu).astype(BF)
    dg_ref[...] = (g * up * (sig + silu * (1 - sig))).astype(BF)


def hidden(b, dy, wg, wu, wd):
    t, d = b.shape
    f = wg.shape[1]
    n = 512
    whole = pl.BlockSpec((t, d), lambda i: (0, 0))
    cols, rows, out = pl.BlockSpec((d, n), lambda i: (0, i)), pl.BlockSpec((n, d), lambda i: (i, 0)), pl.BlockSpec((t, n), lambda i: (0, i))
    return pl.pallas_call(
        _hidden_body, grid=(f // n,), in_specs=[whole, whole, cols, cols, rows], out_specs=[out] * 3, out_shape=[_like((t, f))] * 3, name="hidden",
        compiler_params=_params("arbitrary"), cost_estimate=_cost(6 * t * d * f, b, dy, wg, wu, wd))(b, dy, wg, wu, wd)


def _pair_bwd_body(n, *refs):
    out_ref = refs[-1]
    total = _dot(refs[0][...], refs[n][...], 1, 1)
    for i in range(1, n):
        total = total + _dot(refs[i][...], refs[n + i][...], 1, 1)
    if len(refs) > 2 * n + 1:
        total = total + refs[2 * n][...].astype(F32)
    out_ref[...] = total.astype(BF)


def pair_bwd(gs, ws, more=None):
    t, f = gs[0].shape
    d = ws[0].shape[0]
    n = 512
    whole = pl.BlockSpec((t, f), lambda i: (0, 0))
    cols, out = pl.BlockSpec((n, f), lambda i: (i, 0)), pl.BlockSpec((t, n), lambda i: (0, i))
    given = [*gs, *ws] + ([] if more is None else [more])
    return pl.pallas_call(
        functools.partial(_pair_bwd_body, len(gs)), grid=(d // n,), in_specs=[whole] * len(gs) + [cols] * len(ws) + ([] if more is None else [out]),
        out_specs=out, out_shape=_like((t, d)), name="hidden_bwd", compiler_params=_params("arbitrary"),
        cost_estimate=_cost(2 * t * d * f * len(gs), *given))(*given)


def _qkv_bwd_body(at_ref, dq_ref, dk_ref, dv_ref, wq_ref, wk_ref, wv_ref, *rest):
    out_ref = rest[-1]
    total = _dot(dq_ref[...], wq_ref[...], 1, 1) + _dot(dk_ref[...], wk_ref[...], 1, 1) + _dot(dv_ref[...], wv_ref[...], 1, 1)
    if len(rest) > 1:
        total = total + rest[0][...].astype(F32)
    out_ref[...] = total.astype(BF)


def qkv_bwd(at, gs, ws, t, more=None):
    n = gs[0].shape[1]
    d = ws[0].shape[0]
    rows = 256
    per = t // rows
    piece = pl.BlockSpec((rows, n), lambda i, at: (at[0] * per + i, 0))
    whole = pl.BlockSpec((d, n), lambda i, at: (0, 0))
    out = pl.BlockSpec((rows, d), lambda i, at: (i, 0))
    given = [*gs, *ws] + ([] if more is None else [more])
    grid_spec = pltpu.PrefetchScalarGridSpec(
        num_scalar_prefetch=1, grid=(per,), in_specs=[piece] * 3 + [whole] * 3 + ([] if more is None else [out]), out_specs=out)
    return pl.pallas_call(_qkv_bwd_body, grid_spec=grid_spec, out_shape=_like((t, d)), name="qkv_bwd", compiler_params=_params("arbitrary"),
                          cost_estimate=_cost(6 * t * d * n, *given))(at, *given)


def _by_weight_body(nl, nr, *refs):
    ls, rs, out_ref = refs[:nl], refs[nl : nl + nr], refs[-1]
    per = ls[0].shape[0]
    total = None
    for s in range(nl):
        r_ref = rs[s * nr // nl]
        at = s * per % r_ref.shape[0]
        term = _dot(ls[s][...], r_ref[at : at + per, :], 0, 0)
        total = term if total is None else total + term
    out_ref[...] = total.astype(BF)


def by_weight(ls, rs, bi, bj):
    t, i = ls[0].shape
    j = rs[0].shape[1]
    return pl.pallas_call(
        functools.partial(_by_weight_body, len(ls), len(rs)), grid=(i // bi, j // bj),
        in_specs=[pl.BlockSpec((l.shape[0], bi), lambda i, j: (0, i)) for l in ls] + [pl.BlockSpec((r.shape[0], bj), lambda i, j: (0, j)) for r in rs],
        out_specs=pl.BlockSpec((bi, bj), lambda i, j: (i, j)), out_shape=_like((i, j)), name="by_weight",
        compiler_params=_params("arbitrary", "arbitrary"), cost_estimate=_cost(2 * t * len(ls) * i * j, *ls, *rs))(*ls, *rs)


def _by_qkv_body(at_ref, *refs):
    ls, rs, outs = refs[:TP], refs[TP : TP + 3], refs[TP + 3 :]
    per = ls[0].shape[0]
    for r_ref, out_ref in zip(rs, outs):
        total = None
        for s in range(TP):
            term = _dot(ls[s][...], r_ref[pl.ds(pl.multiple_of(at_ref[s] * per, per), per), :], 0, 0)
            total = term if total is None else total + term
        out_ref[...] = total.astype(BF)


def by_qkv(at, ls, gs, bi=512):
    t, i = ls[0].shape
    total, n = gs[0].shape
    grid_spec = pltpu.PrefetchScalarGridSpec(
        num_scalar_prefetch=1, grid=(i // bi,),
        in_specs=[pl.BlockSpec((t, bi), lambda i, at: (0, i))] * TP + [pl.BlockSpec((total, n), lambda i, at: (0, 0))] * 3,
        out_specs=[pl.BlockSpec((bi, n), lambda i, at: (i, 0))] * 3)
    return pl.pallas_call(_by_qkv_body, grid_spec=grid_spec, out_shape=[_like((i, n))] * 3, name="by_qkv", compiler_params=_params("arbitrary"),
                          cost_estimate=_cost(6 * total * i * n, *ls, *gs))(at, *ls, *gs)


def _by_out_body(at_ref, o_ref, *refs):
    rs, out_ref = refs[:TP], refs[TP]
    per = rs[0].shape[0]
    total = None
    for s in range(TP):
        term = _dot(o_ref[pl.ds(pl.multiple_of(at_ref[s] * per, per), per), :], rs[s][...], 0, 0)
        total = term if total is None else total + term
    out_ref[...] = total.astype(BF)


def by_out(at, o, rs, bj=512):
    total, n = o.shape
    t, d = rs[0].shape
    grid_spec = pltpu.PrefetchScalarGridSpec(
        num_scalar_prefetch=1, grid=(d // bj,),
        in_specs=[pl.BlockSpec((total, n), lambda j, at: (0, 0))] + [pl.BlockSpec((t, bj), lambda j, at: (0, j))] * TP,
        out_specs=pl.BlockSpec((n, bj), lambda j, at: (0, j)))
    return pl.pallas_call(_by_out_body, grid_spec=grid_spec, out_shape=_like((n, d)), name="by_out", compiler_params=_params("arbitrary"),
                          cost_estimate=_cost(2 * total * d * n, o, *rs))(at, o, *rs)


def swap(x, s):
    return lax.ppermute(x, "tp", [(i, i ^ s) for i in range(TP)])


def gather(x):
    half = x.shape[0] // 2
    fx, fy = swap(x, 4), swap(x, 2)
    out = {0: x, 1: swap(x, 1), 4: fx, 2: fy}
    out[6] = jnp.concatenate([swap(fx[:half], 2), swap(fy[half:], 4)])
    for s in (4, 2, 6):
        out[s + 1] = swap(out[s], 1)
    return [out[s] for s in range(TP)]


def plus(a, b):
    return (a.astype(F32) + b.astype(F32)).astype(BF)


def scatter(term):
    mine = {}
    for s in (4, 2, 6, 0):
        mine[s] = term(s, swap(term(s + 1, None), 1))
    half = mine[0].shape[0] // 2
    x0, y1 = swap(mine[4][:half], 4), swap(mine[2][half:], 2)
    dx, dy = swap(mine[6][:half], 4), swap(mine[6][half:], 2)
    x1 = swap(plus(mine[4][half:], dy), 4)
    y0 = swap(plus(mine[2][:half], dx), 2)
    return [mine[0], jnp.concatenate([x0, x1]), jnp.concatenate([y0, y1])]


def tables(tokens):
    half = HEAD // 2
    angle = jnp.arange(tokens, dtype=F32)[:, None] * THETA ** (-jnp.arange(half, dtype=F32) / half)
    cos, sin = jnp.cos(angle), jnp.sin(angle)
    return jnp.concatenate([cos, cos], 1), jnp.concatenate([-sin, sin], 1)


ORDER = (0, 1, 4, 5, 2, 3, 6, 7)


def layer(x, dy, wq, wk, wv, wo, wg, wu, wd):
    me = lax.axis_index("tp")
    t = x.shape[0]
    at = jnp.bitwise_xor(me, jnp.arange(TP, dtype=jnp.int32))
    cos, sin = tables(TP * t)
    a = gather(norm(x))
    before = ()
    for s in ORDER:
        before = qkv(at[s : s + 1], a[s], wq, wk, wv, cos, sin, before)
    q, k, v = before
    wos = gather(wo)
    dys = gather(dy)
    o, lse = attend(q, k, v)
    pieces = [lax.dynamic_slice_in_dim(o, at[s] * t, t, 0) for s in range(TP)]
    os = [pieces[0]] + [swap(pieces[s], s) for s in range(1, TP)]
    h, b = out_proj(os, wos, x)
    bs = gather(b)
    grads = {s: hidden(bs[s], dys[s], wg, wu, wd) for s in ORDER}
    db = scatter(lambda s, more: pair_bwd(grads[s][1:], (wg, wu), more))
    hids, dgs, dus = ([grads[s][n] for s in range(TP)] for n in range(3))
    by_down = by_weight(hids, dys, 512, 512)
    by_gate = by_weight(bs, dgs, 512, 512)
    by_up = by_weight(bs, dus, 512, 512)
    dh = norm_bwd(h, dy, db)
    back = out_proj_bwd(dh, wos)
    dos = [back[0]] + [swap(back[s], s) for s in range(1, TP)]
    do = jnp.zeros(o.shape, BF)
    for s in range(TP):
        do = lax.dynamic_update_slice_in_dim(do, dos[s], at[s] * t, 0)
    dhs = gather(dh)
    dq, dk, dv = attend_bwd(q, k, v, do, o, lse, cos, sin)
    da = scatter(lambda s, more: qkv_bwd(at[s : s + 1], (dq, dk, dv), (wq, wk, wv), t, more))
    by_q, by_k, by_v = by_qkv(at, a, (dq, dk, dv))
    by_o = by_out(at, o, dhs)
    dx = norm_bwd(x, dh, da)
    return dx, by_q, by_k, by_v, by_o, by_gate, by_up, by_down


def solution(mesh):
    def step(x, dy, *weights):
        dx, *rest = layer(x[0], dy[0], *weights)
        return (dx[None], *rest)

    states, by_columns, by_rows = P("dp", "tp", None), P(None, "tp"), P("tp", None)
    weights = (by_columns, by_columns, by_columns, by_rows, by_columns, by_columns, by_rows)
    own = tuple(P("dp", "tp") if spec == by_columns else P(("dp", "tp"), None) for spec in weights)
    return jax.shard_map(step, mesh=mesh, in_specs=(states, states, *weights), out_specs=(states, *own), check_vma=False)
```

```python
import functools

import jax
import jax.numpy as jnp
from jax import lax
from jax.experimental import pallas as pl
from jax.experimental.pallas import tpu as pltpu
from jax.sharding import PartitionSpec as P


HEAD = 128
THETA = 10000
NEG = -1e30
HIDDEN = 2 * NEG
LOG2E = 1.4426950408889634
VMEM = 66 * 10**6
BF = jnp.bfloat16
F32 = jnp.float32
TP = 8
PAIRS = 4
ME, C, Y, YC, X, XC, D, DC = range(TP)
BY_DISTANCE = (DC, D, XC, YC, X, Y, C)
ROWS = 64


def _dot(a, b, ca=1, cb=0):
    return lax.dot_general(a, b, (((ca,), (cb,)), ((), ())), preferred_element_type=F32)


def _dot_t(a, b):
    return _dot(a, b, 1, 1)


def _at(start, size):
    return pl.ds(pl.multiple_of(start, size), size)


def _rows(n, size, start=0):
    return lambda body: pl.loop(0, n // size)(lambda i: body(_at(start + i * size, size)))


def _talks(number, name, **more):
    params = pltpu.CompilerParams(vmem_limit_bytes=VMEM, collective_id=number, has_side_effects=True, **more)
    return {"compiler_params": params, "name": name}


ANY = pl.BlockSpec(memory_space=pl.ANY)
SEMS = pltpu.SemaphoreType.DMA((TP,))


def _vmem(*shape, dtype=BF):
    return pltpu.VMEM(shape, dtype)


def _like(shape, dtype=BF):
    return jax.ShapeDtypeStruct(shape, dtype)


class Links:
    def __init__(self):
        self.me = lax.axis_index("tp")
        self.steps = {n: n - 2 * n * lax.rem(lax.div(self.me, n), 2) for n in (C, Y, X)}
        self.c, self.y, self.x = (self.me + step for step in self.steps.values())

    def owner(self, s):
        place = self.me
        for n, step in self.steps.items():
            place = place + (step * (s // n % 2) if isinstance(s, int) else step * lax.rem(lax.div(s, n), 2))
        return place

    def meet(self):
        barrier = pltpu.get_barrier_semaphore()
        for d in (self.c, self.y, self.x):
            pl.semaphore_signal(barrier, inc=1, device_id={"tp": d}, device_id_type=pl.DeviceIdType.MESH)
        pl.semaphore_wait(barrier, 3)

    def meet_all(self):
        barrier = pltpu.get_barrier_semaphore()
        for s in range(1, TP):
            pl.semaphore_signal(barrier, inc=1, device_id={"tp": self.owner(s)}, device_id_type=pl.DeviceIdType.MESH)
        pl.semaphore_wait(barrier, TP - 1)


def _remote(src, dst, send, recv, to):
    return pltpu.make_async_remote_copy(src_ref=src, dst_ref=dst, send_sem=send, recv_sem=recv, device_id={"tp": to},
                                        device_id_type=pl.DeviceIdType.MESH)


class Gather:
    def __init__(self, links, own, every, send, recv, far=True):
        h = own.shape[0] // 2
        lo, hi = pl.ds(0, h), pl.ds(h, h)
        k = links
        routes = [(own, every.at[C], k.c), (own, every.at[X], k.x), (own, every.at[Y], k.y), (every.at[X, lo], every.at[D, lo], k.y),
                  (every.at[Y, hi], every.at[D, hi], k.x), (every.at[X], every.at[XC], k.c), (every.at[Y], every.at[YC], k.c),
                  (every.at[D], every.at[DC], k.c)]
        self.copies = {n: _remote(src, dst, send.at[n], recv.at[n], to) for n, (src, dst, to) in enumerate(routes) if far or n not in (3, 4, 7)}

    def begin(self):
        for n in (1, 2, 0):
            self.copies[n].start()

    def got(self, *ns):
        for n in ns:
            self.copies[n].wait_recv()

    def middle(self):
        self.got(1, 2)
        for n in (3, 4, 5, 6):
            if n in self.copies:
                self.copies[n].start()

    def far(self):
        self.got(3, 4)
        self.copies[7].start()

    def end(self):
        for c in self.copies.values():
            c.wait_send()


class Far:
    def __init__(self, links, every, far, send, recv):
        h = far.shape[1] // 2
        lo, hi = pl.ds(0, h), pl.ds(h, h)
        self.copies = [_remote(every.at[X, lo], far.at[0, lo], send.at[0], recv.at[0], links.y),
                       _remote(every.at[Y, hi], far.at[0, hi], send.at[1], recv.at[1], links.x),
                       _remote(far.at[0], far.at[1], send.at[2], recv.at[2], links.c)]

    def begin(self):
        self.copies[0].start()
        self.copies[1].start()

    def got(self, *ns):
        for n in ns:
            self.copies[n].wait_recv()

    def turn(self):
        self.got(0, 1)
        self.copies[2].start()

    def end(self):
        for c in self.copies:
            c.wait_send()


class Scatter:
    def __init__(self, links, term, back, sums, via_x, via_y, from_x, from_y, send, recv, free):
        h = term.shape[0] // 2
        lo, hi = pl.ds(0, h), pl.ds(h, h)
        k = links
        self.links, self.free, self.h = k, free, h
        self.sums, self.via_x, self.via_y = sums, via_x, via_y
        self.pair = _remote(term, back, send.at[0], recv.at[0], k.c)
        routes = [(sums.at[1, lo], from_x.at[lo], k.x), (sums.at[2, hi], from_y.at[hi], k.y), (sums.at[3, lo], via_x, k.x),
                  (sums.at[3, hi], via_y, k.y), (sums.at[1, hi], from_x.at[hi], k.x), (sums.at[2, lo], from_y.at[lo], k.y)]
        self.copies = [_remote(src, dst, send.at[n + 1], recv.at[n + 1], to) for n, (src, dst, to) in enumerate(routes)]

    def room(self, j):
        @pl.when(j > 0)
        def _():
            self.pair.wait_send()

    def give(self, j):
        @pl.when(j > 0)
        def _():
            pl.semaphore_wait(self.free, 1)

        self.pair.start()

    def take(self):
        self.pair.wait_recv()

    def taken(self, j):
        @pl.when(j < 3)
        def _():
            pl.semaphore_signal(self.free, inc=1, device_id={"tp": self.links.c}, device_id_type=pl.DeviceIdType.MESH)

    def pass_on(self, pi):
        for n, at in ((0, 1), (1, 2), (2, 3), (3, 3)):

            @pl.when(pi == at)
            def _(n=n):
                self.copies[n].start()

    def finish(self):
        for n, via, pair, start in ((2, self.via_x, 2, 0), (3, self.via_y, 1, self.h)):
            self.copies[n].wait_recv()

            @_rows(self.h, ROWS)
            def _(here):
                at = _at(start + here.start, ROWS)
                self.sums[pair, at, :] = (self.sums[pair, at, :].astype(F32) + via[here, :].astype(F32)).astype(BF)

            self.copies[5 if pair == 2 else 4].start()

    def end(self, pair=True):
        if pair:
            self.pair.wait_send()
        for n in (0, 1, 4, 5):
            self.copies[n].wait_recv()
        for c in self.copies:
            c.wait_send()


def _scale_of(wide):
    return lax.rsqrt(jnp.mean(wide * wide, -1, keepdims=True) + 1e-6)


def _norm_bwd_body(n, h_ref, base_ref, *rest):
    out_ref = rest[n]
    g = rest[0][...].astype(F32)
    for r in rest[1:n]:
        g = g + r[...].astype(F32)
    wide = h_ref[...].astype(F32)
    scale = _scale_of(wide)
    along = jnp.mean(g * wide, -1, keepdims=True)
    out_ref[...] = (base_ref[...].astype(F32) + scale * (g - wide * (scale * scale * along))).astype(BF)


def norm_bwd(h, base, terms):
    t, d = h.shape
    rows = 128
    spec = pl.BlockSpec((rows, d), lambda i: (i, 0))
    return pl.pallas_call(functools.partial(_norm_bwd_body, len(terms)), grid=(t // rows,), in_specs=[spec] * (2 + len(terms)), out_specs=spec,
                          out_shape=_like(h.shape), name="norm_bwd", compiler_params=pltpu.CompilerParams(vmem_limit_bytes=VMEM))(h, base, *terms)


def _turn(x, cos, sin):
    parts = [x[:, n : n + HEAD] for n in range(0, x.shape[1], HEAD)]
    return jnp.concatenate([p * cos + pltpu.roll(p, HEAD // 2, 1) * sin for p in parts], axis=1)


def _diagonal(size):
    return lax.broadcasted_iota(jnp.int32, (size, size), 1) >= lax.broadcasted_iota(jnp.int32, (size, size), 0)


def _attend_body(q_ref, k_ref, v_ref, wo_ref, o_ref, lse_ref, wos_ref, top_s, mix_s, send, recv, *, scale, b):
    links = Links()
    gather = Gather(links, wo_ref, wos_ref, send, recv)

    @pl.when(pl.program_id(0) == 0)
    def _():
        links.meet()
        gather.begin()

    bq, width = q_ref.shape
    heads, strips = width // HEAD, bq // b
    iq = pl.program_id(0)
    e = scale * LOG2E
    top_s[...] = jnp.full_like(top_s, NEG)
    mix_s[...] = jnp.zeros_like(mix_s)
    ones = jnp.ones((8, b), BF)

    def block(j, first):
        here = pl.ds(j * b, b)
        pieces = [(i, n) for i in range(heads) for n in range(first or 0, strips)]
        scores = [_dot_t(k_ref[here, i * HEAD : (i + 1) * HEAD], q_ref[n * b : (n + 1) * b, i * HEAD : (i + 1) * HEAD]) for i, n in pieces]
        weights, keeps = [], []
        for (i, n), s in zip(pieces, scores):
            if n == first:
                s = jnp.where(_diagonal(b), s, HIDDEN)
            at = slice(n * b, (n + 1) * b)
            old = top_s[i : i + 1, at]
            top = jnp.maximum(old, s.max(axis=0, keepdims=True))
            top_s[i : i + 1, at] = top
            weights.append(jnp.exp2((s - top) * e).astype(BF))
            keeps.append(jnp.exp2((old - top) * e))
        for (i, n), p, keep in zip(pieces, weights, keeps):
            at = slice(n * b, (n + 1) * b)
            values = jnp.concatenate([v_ref[here, i * HEAD : (i + 1) * HEAD].T, ones], axis=0)
            mix_s[i, :, at] = mix_s[i, :, at] * keep + _dot(values, p)

    lax.fori_loop(0, iq * strips, lambda j, _: block(j, None), None)

    @pl.when(iq == 1)
    def _():
        gather.middle()

    for n in range(strips):
        block(iq * strips + n, n)
    for i in range(heads):
        total = mix_s[i, HEAD : HEAD + 1, :]
        o_ref[:, i * HEAD : (i + 1) * HEAD] = (mix_s[i, :HEAD, :] * (1 / total)).T.astype(BF)
        lse_ref[i : i + 1, :] = top_s[i : i + 1, :] * scale + jnp.log(total)

    @pl.when(iq == pl.num_programs(0) - 1)
    def _():
        gather.far()
        gather.got(0, 5, 6, 7)
        gather.end()


def attend(q, k, v, wo, bq=2048, b=512):
    t, n = q.shape
    heads = n // HEAD
    whole = pl.BlockSpec((t, n), lambda i: (0, 0))
    rows = pl.BlockSpec((bq, n), lambda i: (i, 0))
    return pl.pallas_call(
        functools.partial(_attend_body, scale=HEAD**-0.5, b=b), grid=(t // bq,), in_specs=[rows, whole, whole, ANY],
        out_specs=[rows, pl.BlockSpec((heads, bq), lambda i: (0, i)), ANY],
        out_shape=[_like((t, n)), _like((heads, t), F32), _like((TP, *wo.shape))],
        scratch_shapes=[_vmem(heads, bq, dtype=F32), _vmem(heads, HEAD + 8, bq, dtype=F32), SEMS, SEMS],
        **_talks(6, "attend", dimension_semantics=("arbitrary",)))(q, k, v, wo)


def _attend_bwd_body(q_ref, k_ref, v_ref, do_ref, o_ref, lse_ref, cosq_ref, sinq_ref, cos_ref, sin_ref, dh_ref, dq_ref, dk_ref, dv_ref, dhs_ref,
                     dq_s, dk_s, dv_s, send, recv, *, scale, b):
    links = Links()
    gather = Gather(links, dh_ref, dhs_ref, send, recv, False)
    bq, width = q_ref.shape
    heads, strips = width // HEAD, bq // b
    iq = pl.program_id(0)
    e = scale * LOG2E

    @pl.when(iq == 0)
    def _():
        links.meet()
        gather.begin()
        dk_s[...] = jnp.zeros_like(dk_s)
        dv_s[...] = jnp.zeros_like(dv_s)

    dq_s[...] = jnp.zeros_like(dq_s)
    lses = [lse_ref[i : i + 1, :] * LOG2E for i in range(heads)]
    deltas = []
    for i in range(heads):
        at = slice(i * HEAD, (i + 1) * HEAD)
        deltas.append((do_ref[:, at].astype(F32) * o_ref[:, at].astype(F32)).T.sum(axis=0, keepdims=True))

    def block(j, first):
        here = pl.ds(j * b, b)
        pieces = [(i, n) for i in range(heads) for n in range(first or 0, strips)]
        qs = [q_ref[n * b : (n + 1) * b, i * HEAD : (i + 1) * HEAD] for i, n in pieces]
        dos = [do_ref[n * b : (n + 1) * b, i * HEAD : (i + 1) * HEAD] for i, n in pieces]
        scores = [_dot_t(k_ref[here, i * HEAD : (i + 1) * HEAD], x) for (i, _), x in zip(pieces, qs)]
        dps = [_dot_t(v_ref[here, i * HEAD : (i + 1) * HEAD], x) for (i, _), x in zip(pieces, dos)]
        for m, (i, n) in enumerate(pieces):
            at, head = slice(n * b, (n + 1) * b), slice(i * HEAD, (i + 1) * HEAD)
            p = jnp.exp2(scores[m] * e - lses[i][:, at])
            if n == first:
                p = jnp.where(_diagonal(b), p, 0.0)
            ds = (p * (dps[m] - deltas[i][:, at])).astype(BF)
            dv_s[here, head] += _dot(p.astype(BF), dos[m])
            dk_s[here, head] += _dot(ds, qs[m])
            dq_s[i, :, at] += _dot(k_ref[here, head].T, ds)

    lax.fori_loop(0, iq * strips, lambda j, _: block(j, None), None)

    @pl.when(iq == pl.num_programs(0) - 1)
    def _():
        gather.middle()

    for n in range(strips):
        block(iq * strips + n, n)

    def back(g, cos, sin):
        return _turn(g.astype(BF).astype(F32), cos, -sin).astype(BF)

    for i in range(heads):
        head = slice(i * HEAD, (i + 1) * HEAD)
        dq_ref[:, head] = back((dq_s[i] * scale).T, cosq_ref[...], sinq_ref[...])

    @pl.when(iq == pl.num_programs(0) - 1)
    def _():
        for i in range(heads):
            head = slice(i * HEAD, (i + 1) * HEAD)
            for r in range(0, dk_s.shape[0], b):
                rows = slice(r, r + b)
                dk_ref[rows, head] = back(dk_s[rows, head] * scale, cos_ref[rows, :], sin_ref[rows, :])
                dv_ref[rows, head] = dv_s[rows, head].astype(BF)
        gather.got(0, 5, 6)
        gather.end()


def attend_bwd(q, k, v, do, o, lse, cos, sin, dh, bq=1024, b=512):
    t, n = q.shape
    heads = n // HEAD
    whole = pl.BlockSpec((t, n), lambda i: (0, 0))
    rows = pl.BlockSpec((bq, n), lambda i: (i, 0))
    part = pl.BlockSpec((bq, HEAD), lambda i: (i, 0))
    table = pl.BlockSpec((t, HEAD), lambda i: (0, 0))
    return pl.pallas_call(
        functools.partial(_attend_bwd_body, scale=HEAD**-0.5, b=b), grid=(t // bq,),
        in_specs=[rows, whole, whole, rows, rows, pl.BlockSpec((heads, bq), lambda i: (0, i)), part, part, table, table, ANY],
        out_specs=[rows, whole, whole, ANY], out_shape=[_like((t, n))] * 3 + [_like((TP, *dh.shape))],
        scratch_shapes=[_vmem(heads, HEAD, bq, dtype=F32), _vmem(t, n, dtype=F32), _vmem(t, n, dtype=F32), SEMS, SEMS],
        **_talks(7, "attend_bwd", dimension_semantics=("arbitrary",)))(q, k, v, do, o, lse, cos, sin, cos, sin, dh)


def _mlp_body(own_ref, dy_ref, dys_ref, wg_hbm, wu_hbm, wd_hbm, all_ref, far_ref, hid_ref, c0_ref, from_x, from_y, bg_ref, bu_ref,
              wg, wu, wd, by_g, by_u, bv, yv, term, back, sums, via_x, via_y, hid, dg, du, load, store, wsem, gsend, grecv, fsend, frecv, ssend, srecv, free):
    k = Links()
    t, d = own_ref.shape
    f = wg.shape[1]
    n = 512
    weights = [pltpu.make_async_copy(a, b, wsem.at[i]) for i, (a, b) in enumerate(((wg_hbm, wg), (wu_hbm, wu), (wd_hbm, wd)))]
    for w in weights:
        w.start()
    k.meet()
    gather = Gather(k, own_ref, all_ref, gsend, grecv)
    scatter = Scatter(k, term, back, sums, via_x, via_y, from_x, from_y, ssend, srecv, free)
    gather.begin()
    far = Far(k, dys_ref, far_ref, fsend, frecv)

    def fetch(s, par):
        y = dy_ref if s == 0 else far_ref.at[s - D] if s >= D else dys_ref.at[s]
        return [pltpu.make_async_copy(all_ref.at[s] if s else own_ref, bv.at[par], load.at[par]),
                pltpu.make_async_copy(y, yv.at[par], load.at[2 + par])]

    def start(copies):
        for c in copies:
            c.start()

    def wait(copies):
        for c in copies:
            c.wait()

    start(fetch(0, 1))
    by_g[...] = jnp.zeros_like(by_g)
    by_u[...] = jnp.zeros_like(by_u)
    gather.got(0)
    start(fetch(1, 0))
    for w in weights:
        w.wait()

    def put(s):
        return pltpu.make_async_copy(hid, hid_ref.at[s], store.at[0])

    def work(s, par, first):
        wait(fetch(1, par))

        @pl.when(jnp.logical_not(first))
        def _():
            put(0).wait()

        @_rows(f, n)
        def _(cols):
            b = bv[par]
            gate, up = _dot(b, wg[:, cols]), _dot(b, wu[:, cols])
            g = _dot_t(yv[par], wd[cols, :]).astype(BF).astype(F32)
            sig = 1 / (1 + jnp.exp(-gate))
            silu = gate * sig
            hid[:, cols] = (silu * up).astype(BF)
            du[:, cols] = (g * silu).astype(BF)
            dg[:, cols] = (g * up * (sig + silu * (1 - sig))).astype(BF)

        put(s).start()

        @_rows(d, f)
        def _(rows):
            bt = bv[par, :, rows].T
            by_g[rows, :] += _dot(bt, dg[...])
            by_u[rows, :] += _dot(bt, du[...])

    def terms(cols):
        return _dot_t(dg[...], wg[cols, :]) + _dot_t(du[...], wu[cols, :])

    @pl.loop(0, PAIRS)
    def _(pi):
        base = 4 * lax.rem(pi, 2) + 2 * lax.div(pi, 2)
        work(base + 1, 0, pi == 0)
        for at, coming, ready in ((1, YC, 6), (2, DC, 7)):

            @pl.when(pi == at)
            def _(coming=coming, ready=ready):
                gather.got(ready)
                if coming == DC:
                    far.got(2)
                start(fetch(coming, 0))

        scatter.room(pi)

        @_rows(d, n)
        def _(cols):
            term[:, cols] = terms(cols).astype(BF)

        scatter.give(pi)
        work(base, 1, pi < 0)

        @pl.when(pi == 0)
        def _():
            gather.middle()
            far.begin()
            start(fetch(X, 1))

        @pl.when(pi == 1)
        def _():
            start(fetch(Y, 1))
            gather.far()
            far.turn()

        @pl.when(pi == 2)
        def _():
            start(fetch(D, 1))

        scatter.take()

        @_rows(d, n)
        def _(cols):
            sums[pi, :, cols] = (terms(cols) + back[:, cols].astype(F32)).astype(BF)

        scatter.taken(pi)
        scatter.pass_on(pi)

        @pl.when(pi == 0)
        def _():
            gather.got(5)
            start(fetch(XC, 0))

    put(0).wait()
    first = pltpu.make_async_copy(sums.at[0], c0_ref, store.at[1])
    first.start()
    slots = (dg, du)
    blocks = [(acc, out, r) for acc, out in ((by_g, bg_ref), (by_u, bu_ref)) for r in range(0, d, t)]

    def leave(m):
        acc, out, r = blocks[m]
        return pltpu.make_async_copy(slots[m % 2], out.at[pl.ds(r, t), :], load.at[m % 2])

    def stage(m):
        acc, out, r = blocks[m]
        if m >= 2:
            leave(m - 2).wait()

        @_rows(t, ROWS)
        def _(here):
            slots[m % 2][here, :] = acc[_at(r + here.start, ROWS), :].astype(BF)

        leave(m).start()

    for m in range(len(blocks)):
        stage(m)
        if m == len(blocks) // 2:
            scatter.finish()
    for m in range(len(blocks) - 2, len(blocks)):
        leave(m).wait()
    first.wait()
    gather.end()
    far.end()
    scatter.end()


def mlp(b, dy, dys, wg, wu, wd):
    t, d = b.shape
    f = wg.shape[1]
    all_, far, hid, c0, fx, fy, bg, bu = pl.pallas_call(
        _mlp_body, in_specs=[ANY] * 6, out_specs=[ANY] * 8,
        out_shape=[_like((TP, t, d)), _like((2, t, d)), _like((TP, t, f))] + [_like((t, d))] * 3 + [_like((d, f))] * 2,
        scratch_shapes=[*[_vmem(d, f)] * 2, _vmem(f, d), *[_vmem(d, f, dtype=F32)] * 2, *[_vmem(2, t, d)] * 2, *[_vmem(t, d)] * 2, _vmem(PAIRS, t, d),
                        *[_vmem(t // 2, d)] * 2, *[_vmem(t, f)] * 3, *[SEMS] * 9, pltpu.SemaphoreType.REGULAR],
        **_talks(1, "mlp"))(b, dy, dys, wg, wu, wd)
    return hid, far, [c0, fx, fy], bg, bu


def _front_body(x_ref, dy_ref, wq_ref, wk_ref, wv_ref, base_ref, fine_ref, all_ref, dys_ref, q_ref, k_ref, v_ref, cos_ref, sin_ref,
                w, xv, av, out, cos, sin, load, store, wsem, asend, arecv, ysend, yrecv):
    k = Links()
    t, d = x_ref.shape
    n = wq_ref.shape[1]
    get = pltpu.make_async_copy(x_ref, xv, load.at[0])
    get.start()
    ws = [pltpu.make_async_copy(r, w.at[:, pl.ds(i * n, n)], wsem.at[i]) for i, r in enumerate((wq_ref, wk_ref, wv_ref))]
    for c in ws:
        c.start()
    get.wait()

    @_rows(t, ROWS)
    def _(at):
        wide = xv[at, :].astype(F32)
        av[0, at, :] = (wide * _scale_of(wide)).astype(BF)

    own = pltpu.make_async_copy(av.at[0], all_ref.at[0], store.at[0])
    own.start()
    k.meet()
    own.wait()
    a = Gather(k, all_ref.at[0], all_ref, asend, arecv)
    y = Gather(k, dy_ref, dys_ref, ysend, yrecv, False)
    a.begin()

    def fetch(s, par):
        return pltpu.make_async_copy(all_ref.at[s], av.at[par], load.at[par])

    def puts(s, par):
        rows = _at(k.owner(s) * t, t)
        return [pltpu.make_async_copy(out.at[par, :, pl.ds(i * n, n)], r.at[rows, :], store.at[3 * par + i]) for i, r in enumerate((q_ref, k_ref, v_ref))]

    def work(s, par, again):
        fetch(s, par).wait()

        @pl.when(again)
        def _():
            for c in puts(s, par):
                c.wait()

        place = k.owner(s)
        bc, bs = base_ref[0, pl.ds(place, 1), :], base_ref[1, pl.ds(place, 1), :]
        sign = jnp.where(lax.broadcasted_iota(jnp.int32, (1, HEAD), 1) < HEAD // 2, -1.0, 1.0)

        got = _dot(av[par], w[...]).astype(BF)
        here = _at(place * t, t)
        fc, fs = fine_ref[0], fine_ref[1]
        c, sn = bc * fc - bs * fs, sign * (bs * fc + bc * fs)
        cos[here, :] = c
        sin[here, :] = sn
        out[par, :, : 2 * n] = _turn(got[:, : 2 * n].astype(F32), c, sn).astype(BF)
        out[par, :, 2 * n :] = got[:, 2 * n :]

        for c in puts(s, par):
            c.start()

    for c in ws:
        c.wait()
    fetch(0, 0).start()

    @pl.loop(0, 4)
    def _(j):
        @pl.when(j == 0)
        def _():
            a.got(0)
            fetch(1, 1).start()

        @pl.when(j == 1)
        def _():
            a.middle()
            y.begin()
            fetch(X, 0).start()
            fetch(Y, 1).start()

        @pl.when(j == 2)
        def _():
            a.got(5, 6)
            fetch(XC, 0).start()
            fetch(YC, 1).start()

        @pl.when(j == 3)
        def _():
            a.far()
            fetch(D, 0).start()
            a.got(7)
            fetch(DC, 1).start()

        work(j + 3 * lax.div(j + 3, 4), 0, j > 0)
        work(j + 1 + 3 * lax.div(j, 3), 1, j > 0)

    turns = [pltpu.make_async_copy(a, b, load.at[i]) for i, (a, b) in enumerate(((cos, cos_ref), (sin, sin_ref)))]
    for c in turns:
        c.start()
    for par in (0, 1):
        for c in puts(6 + par, par):
            c.wait()
    for c in turns:
        c.wait()
    y.middle()
    y.got(0, 5, 6)
    a.end()
    y.end()


def front(x, dy, wq, wk, wv, base, fine):
    t, d = x.shape
    n = wq.shape[1]
    vmem = pl.BlockSpec(memory_space=pltpu.VMEM)
    return pl.pallas_call(
        _front_body, in_specs=[ANY] * 5 + [vmem] * 2, out_specs=[ANY] * 7,
        out_shape=[_like((TP, t, d))] * 2 + [_like((TP * t, n))] * 3 + [_like((TP * t, HEAD), F32)] * 2,
        scratch_shapes=[_vmem(d, 3 * n), _vmem(t, d), _vmem(2, t, d), _vmem(2, t, 3 * n), *[_vmem(TP * t, HEAD, dtype=F32)] * 2, *[SEMS] * 7],
        **_talks(2, "front"))(x, dy, wq, wk, wv, base, fine)


def _join_body(o_ref, wo_ref, wos_ref, x_ref, h_ref, b_ref, os, ws, xv, bv, acc, load, wsem, send, recv):
    k = Links()
    t, d = x_ref.shape
    wl = [pltpu.make_async_copy(wo_ref if s == 0 else wos_ref.at[s], ws.at[s], wsem.at[s]) for s in range(TP)]
    for c in wl:
        c.start()
    rows = lambda s: _at(k.owner(s) * t, t)
    own = pltpu.make_async_copy(o_ref.at[rows(0), :], os.at[0], load.at[0])
    own.start()
    xl = pltpu.make_async_copy(x_ref, xv, load.at[1])
    xl.start()
    k.meet_all()
    copies = {s: _remote(o_ref.at[rows(s), :], os.at[s], send.at[s], recv.at[s], k.owner(s)) for s in range(1, TP)}
    for s in BY_DISTANCE:
        copies[s].start()
    own.wait()
    wl[0].wait()

    def add(s, first):
        got = _dot(os[s], ws[s])
        acc[...] = got if first else acc[...] + got

    add(0, True)
    for s in BY_DISTANCE[::-1]:
        wl[s].wait()
        copies[s].wait_recv()
        add(s, False)
    xl.wait()
    out = []
    for r in range(0, t, 128):

        @_rows(128, ROWS, r)
        def _(at):
            h = (xv[at, :].astype(F32) + acc[at, :].astype(BF).astype(F32)).astype(BF)
            xv[at, :] = h
            wide = h.astype(F32)
            bv[at, :] = (wide * _scale_of(wide)).astype(BF)

        here = pl.ds(r, 128)
        out += [pltpu.make_async_copy(xv.at[here, :], h_ref.at[here, :], wsem.at[len(out)]),
                pltpu.make_async_copy(bv.at[here, :], b_ref.at[here, :], wsem.at[len(out) + 1])]
        out[-2].start()
        out[-1].start()
    for c in out:
        c.wait()
    for c in copies.values():
        c.wait_send()


def join(o, wo, wos, x):
    t, d = x.shape
    n = o.shape[1]
    return pl.pallas_call(
        _join_body, in_specs=[ANY] * 4, out_specs=[ANY] * 2, out_shape=[_like((t, d))] * 2,
        scratch_shapes=[_vmem(TP, t, n), _vmem(TP, n, d), *[_vmem(t, d)] * 2, _vmem(t, d, dtype=F32), *[SEMS] * 4], **_talks(3, "join"))(o, wo, wos, x)


def _part_body(h_ref, dy_ref, c0_ref, fx_ref, fy_ref, wo_ref, wos_ref, dh_ref, do_ref, ws, ins, dh, back, load, wsem, send, recv):
    k = Links()
    t, d = h_ref.shape
    q = 128
    parts = [[pltpu.make_async_copy(r.at[pl.ds(i, q), :], ins.at[m, pl.ds(i, q), :], load.at[m, i // q])
              for m, r in enumerate((h_ref, dy_ref, c0_ref, fx_ref, fy_ref))] for i in range(0, t, q)]
    for p in parts:
        for c in p:
            c.start()
    order = (*BY_DISTANCE, ME)
    wl = {s: pltpu.make_async_copy(wo_ref if s == 0 else wos_ref.at[s], ws.at[s], wsem.at[s]) for s in order}
    for s in order:
        wl[s].start()
    k.meet_all()
    out = []
    for i, p in enumerate(parts):
        for c in p:
            c.wait()

        @_rows(q, 32, i * q)
        def _(at):
            h, base, g, fx, fy = (ins[m, at, :].astype(F32) for m in range(5))
            g = g + fx + fy
            scale = _scale_of(h)
            along = jnp.mean(g * h, -1, keepdims=True)
            dh[at, :] = (base + scale * (g - h * (scale * scale * along))).astype(BF)

        here = pl.ds(i * q, q)
        out.append(pltpu.make_async_copy(dh.at[here, :], dh_ref.at[here, :], load.at[0, i]))
        out[-1].start()
    mine = _at(k.me * t, t)
    copies = {s: _remote(back.at[s], do_ref.at[mine, :], send.at[s], recv.at[s], k.owner(s)) for s in range(1, TP)}
    own = pltpu.make_async_copy(back.at[0], do_ref.at[mine, :], load.at[1, 0])
    for s in order:
        wl[s].wait()
        back[s] = _dot_t(dh[...], ws[s]).astype(BF)
        (copies[s] if s else own).start()
    for c in out:
        c.wait()
    own.wait()
    for c in copies.values():
        c.wait()


def part(h, dy, db, wo, wos):
    t, d = h.shape
    n = wo.shape[0]
    return pl.pallas_call(
        _part_body, in_specs=[ANY] * 7, out_specs=[ANY] * 2, out_shape=[_like((t, d)), _like((TP * t, n))],
        scratch_shapes=[_vmem(TP, n, d), _vmem(5, t, d), _vmem(t, d), _vmem(TP, t, n), pltpu.SemaphoreType.DMA((5, PAIRS)), *[SEMS] * 3],
        **_talks(4, "part"))(h, dy, *db, wo, wos)


def _rear_body(dq_ref, dk_ref, dv_ref, wq_ref, wk_ref, wv_ref, all_ref, o_ref, dh_ref, dhs_ref, hid_ref, dy_ref, dys_ref, far_ref,
               c0_ref, from_x, from_y, bq_ref, bk_ref, bv_ref, bo_ref, bd_ref, end_ref,
               g, w, o, av, hv, iv, yv, by_w, by_o, by_d, term, back, sums, via_x, via_y, load, gsem, wsem, ssend, srecv, esend, erecv, free):
    k = Links()
    n = dq_ref.shape[1]
    _, t, d = all_ref.shape
    f = iv.shape[2]
    gets = [pltpu.make_async_copy(r, g.at[:, pl.ds(i * n, n)], gsem.at[i]) for i, r in enumerate((dq_ref, dk_ref, dv_ref))]
    gets += [pltpu.make_async_copy(r, w.at[:, pl.ds(i * n, n)], wsem.at[i]) for i, r in enumerate((wq_ref, wk_ref, wv_ref))]
    gets.append(pltpu.make_async_copy(o_ref, o, gsem.at[3]))
    for c in gets:
        c.start()
    k.meet()
    scatter = Scatter(k, term, back, sums, via_x, via_y, from_x, from_y, ssend, srecv, free)

    last = Far(k, dhs_ref, end_ref, esend, erecv)
    last.begin()

    def fetch(s, par, h, y):
        return [pltpu.make_async_copy(src, dst.at[par], load.at[m, par])
                for m, (src, dst) in enumerate(((all_ref.at[s], av), (hid_ref.at[s], iv), (h, hv), (y, yv)))]

    def start(s, par):
        @pl.when(s == 0)
        def _():
            for c in fetch(s, par, dh_ref, dy_ref):
                c.start()

        @pl.when(jnp.logical_and(s > 0, s < D))
        def _():
            for c in fetch(s, par, dhs_ref.at[s], dys_ref.at[s]):
                c.start()

        @pl.when(s == D)
        def _():
            last.turn()

        @pl.when(s == DC)
        def _():
            last.got(2)

        @pl.when(s >= D)
        def _():
            for c in fetch(s, par, end_ref.at[lax.rem(s, 2)], far_ref.at[lax.rem(s, 2)]):
                c.start()

    start(0, 0)
    for c in gets:
        c.wait()

    def terms(s, cols):
        return _dot_t(g[_at(k.owner(s) * t, t), :], w[cols, :])

    @pl.loop(0, PAIRS)
    def _(j):
        pi = j + 3 * lax.div(3 - j, 3) - 3 * lax.div(j, 3)
        base = 4 * lax.rem(pi, 2) + 2 * lax.div(pi, 2)
        scatter.room(j)

        @_rows(d, f)
        def _(cols):
            term[:, cols] = terms(base + 1, cols).astype(BF)

        scatter.give(j)
        scatter.take()

        @_rows(d, f)
        def _(cols):
            sums[pi, :, cols] = (terms(base, cols) + back[:, cols].astype(F32)).astype(BF)

        scatter.taken(j)
        scatter.pass_on(pi)

    first = pltpu.make_async_copy(sums.at[0], c0_ref, gsem.at[0])
    first.start()

    for acc in (by_w, by_d, by_o):
        acc[...] = jnp.zeros_like(acc)

    @pl.loop(0, TP)
    def _(s):
        par = lax.rem(s, 2)
        for c in fetch(s, par, dh_ref, dy_ref):
            c.wait()

        @pl.when(s < TP - 1)
        def _():
            start(s + 1, 1 - par)

        here = _at(k.owner(s) * t, t)

        @_rows(d, f)
        def _(rows):
            by_w[rows, :] += _dot(av[par, :, rows].T, g[here, :])

        it = iv[par].T

        @_rows(d, t)
        def _(cols):
            by_d[:, cols] += _dot(it, yv[par, :, cols])

        by_o[...] += _dot(o[here, :].T, hv[par])

        @pl.when(s == 0)
        def _():
            scatter.finish()

    scatter.pair.wait_send()
    outs = []

    def leave(src, dst, sem):
        outs.append(pltpu.make_async_copy(src, dst, sem))
        outs[-1].start()

    @_rows(d, 256)
    def _(rows):
        w[rows, :] = by_w[rows, :].astype(BF)

    for i, r in enumerate((bq_ref, bk_ref, bv_ref)):
        leave(w.at[:, pl.ds(i * n, n)], r, wsem.at[i])
    for i in range(f // t):

        @_rows(t, ROWS)
        def _(rows, i=i):
            av[i, rows, :] = by_d[_at(i * t + rows.start, ROWS), :].astype(BF)

        leave(av.at[i], bd_ref.at[pl.ds(i * t, t), :], load.at[0, i])

    @_rows(n, ROWS)
    def _(rows):
        term[rows, :] = by_o[rows, :].astype(BF)

    leave(term.at[pl.ds(0, n), :], bo_ref, gsem.at[1])
    for c in [*outs, first]:
        c.wait()
    last.end()
    scatter.end(False)


def rear(gs, ws, every, o, dh, dhs, hids, dy, dys, far):
    _, t, d = every.shape
    n, f = ws[0].shape[1], hids.shape[2]
    *terms, bq, bk, bv, bo, bd, _ = pl.pallas_call(
        _rear_body, in_specs=[ANY] * 14, out_specs=[ANY] * 9,
        out_shape=[_like((t, d))] * 3 + [_like((d, n))] * 3 + [_like((n, d)), _like((f, d)), _like((2, t, d))],
        scratch_shapes=[_vmem(TP * t, 3 * n), _vmem(d, 3 * n), _vmem(TP * t, n), *[_vmem(2, t, d)] * 2, _vmem(2, t, f), _vmem(2, t, d),
                        _vmem(d, 3 * n, dtype=F32), _vmem(n, d, dtype=F32), _vmem(f, d, dtype=F32), *[_vmem(t, d)] * 2, _vmem(PAIRS, t, d),
                        *[_vmem(t // 2, d)] * 2, pltpu.SemaphoreType.DMA((PAIRS, 2)), *[SEMS] * 6, pltpu.SemaphoreType.REGULAR],
        **_talks(5, "rear"))(*gs, *ws, every, o, dh, dhs, hids, dy, dys, far)
    return terms, bq, bk, bv, bo, bd


def tables(t):
    half = HEAD // 2

    def of(places):
        angle = places.astype(F32)[:, None] * THETA ** (-jnp.arange(half, dtype=F32) / half)
        return jnp.tile(jnp.stack([jnp.cos(angle), jnp.sin(angle)]), 2)

    return of(jnp.arange(TP) * t), of(jnp.arange(t))


def layer(x, dy, wq, wk, wv, wo, wg, wu, wd):
    every, dys, q, k, v, cos, sin = front(x, dy, wq, wk, wv, *tables(x.shape[0]))
    o, lse, wos = attend(q, k, v, wo)
    h, b = join(o, wo, wos, x)
    hids, far, db, by_gate, by_up = mlp(b, dy, dys, wg, wu, wd)
    dh, do = part(h, dy, db, wo, wos)
    dq, dk, dv, dhs = attend_bwd(q, k, v, do, o, lse, cos, sin, dh)
    da, by_q, by_k, by_v, by_o, by_down = rear((dq, dk, dv), (wq, wk, wv), every, o, dh, dhs, hids, dy, dys, far)
    dx = norm_bwd(x, dh, da)
    return dx, by_q, by_k, by_v, by_o, by_gate, by_up, by_down


def solution(mesh):
    def step(x, dy, *weights):
        dx, *rest = layer(x[0], dy[0], *weights)
        return (dx[None], *rest)

    states, by_columns, by_rows = P("dp", "tp", None), P(None, "tp"), P("tp", None)
    weights = (by_columns, by_columns, by_columns, by_rows, by_columns, by_columns, by_rows)
    own = tuple(P("dp", "tp") if spec == by_columns else P(("dp", "tp"), None) for spec in weights)
    return jax.shard_map(step, mesh=mesh, in_specs=(states, states, *weights), out_specs=(states, *own), check_vma=False)
```

```python
import functools

import jax
import jax.numpy as jnp
from jax import lax
from jax.experimental import pallas as pl
from jax.experimental.pallas import tpu as pltpu
from jax.sharding import PartitionSpec as P


HEAD = 128
THETA = 10000
NEG = -1e30
HIDDEN = 2 * NEG
LOG2E = 1.4426950408889634
VMEM = 66 * 10**6
BF = jnp.bfloat16
F32 = jnp.float32
TP = 8
PAIRS = 4
ME, C, Y, YC, X, XC, D, DC = range(TP)
BY_DISTANCE = (DC, D, XC, YC, X, Y, C)
ROWS = 64


def _dot(a, b, ca=1, cb=0):
    return lax.dot_general(a, b, (((ca,), (cb,)), ((), ())), preferred_element_type=F32)


def _dot_t(a, b):
    return _dot(a, b, 1, 1)


def _at(start, size):
    return pl.ds(pl.multiple_of(start, size), size)


def _rows(n, size, start=0):
    return lambda body: pl.loop(0, n // size)(lambda i: body(_at(start + i * size, size)))


def _talks(number, name, **more):
    params = pltpu.CompilerParams(vmem_limit_bytes=VMEM, collective_id=number, has_side_effects=True, **more)
    return {"compiler_params": params, "name": name}


ANY = pl.BlockSpec(memory_space=pl.ANY)
SEMS = pltpu.SemaphoreType.DMA((TP,))


def _vmem(*shape, dtype=BF):
    return pltpu.VMEM(shape, dtype)


def _like(shape, dtype=BF):
    return jax.ShapeDtypeStruct(shape, dtype)


class Links:
    def __init__(self):
        self.me = lax.axis_index("tp")
        self.steps = {n: n - 2 * n * lax.rem(lax.div(self.me, n), 2) for n in (C, Y, X)}
        self.c, self.y, self.x = (self.me + step for step in self.steps.values())

    def owner(self, s):
        place = self.me
        for n, step in self.steps.items():
            place = place + (step * (s // n % 2) if isinstance(s, int) else step * lax.rem(lax.div(s, n), 2))
        return place

    def meet(self):
        barrier = pltpu.get_barrier_semaphore()
        for d in (self.c, self.y, self.x):
            pl.semaphore_signal(barrier, inc=1, device_id={"tp": d}, device_id_type=pl.DeviceIdType.MESH)
        pl.semaphore_wait(barrier, 3)

    def meet_all(self):
        barrier = pltpu.get_barrier_semaphore()
        for s in range(1, TP):
            pl.semaphore_signal(barrier, inc=1, device_id={"tp": self.owner(s)}, device_id_type=pl.DeviceIdType.MESH)
        pl.semaphore_wait(barrier, TP - 1)


def _remote(src, dst, send, recv, to):
    return pltpu.make_async_remote_copy(src_ref=src, dst_ref=dst, send_sem=send, recv_sem=recv, device_id={"tp": to},
                                        device_id_type=pl.DeviceIdType.MESH)


class Gather:
    def __init__(self, links, own, every, send, recv, far=True):
        h = own.shape[0] // 2
        lo, hi = pl.ds(0, h), pl.ds(h, h)
        k = links
        routes = [(own, every.at[C], k.c), (own, every.at[X], k.x), (own, every.at[Y], k.y), (every.at[X, lo], every.at[D, lo], k.y),
                  (every.at[Y, hi], every.at[D, hi], k.x), (every.at[X], every.at[XC], k.c), (every.at[Y], every.at[YC], k.c),
                  (every.at[D], every.at[DC], k.c)]
        self.copies = {n: _remote(src, dst, send.at[n], recv.at[n], to) for n, (src, dst, to) in enumerate(routes) if far or n not in (3, 4, 7)}

    def begin(self):
        for n in (1, 2, 0):
            self.copies[n].start()

    def got(self, *ns):
        for n in ns:
            self.copies[n].wait_recv()

    def middle(self):
        self.got(1, 2)
        for n in (3, 4, 5, 6):
            if n in self.copies:
                self.copies[n].start()

    def far(self):
        self.got(3, 4)
        self.copies[7].start()

    def end(self):
        for c in self.copies.values():
            c.wait_send()


class Far:
    def __init__(self, links, every, far, send, recv):
        h = far.shape[1] // 2
        lo, hi = pl.ds(0, h), pl.ds(h, h)
        self.copies = [_remote(every.at[X, lo], far.at[0, lo], send.at[0], recv.at[0], links.y),
                       _remote(every.at[Y, hi], far.at[0, hi], send.at[1], recv.at[1], links.x),
                       _remote(far.at[0], far.at[1], send.at[2], recv.at[2], links.c)]

    def begin(self):
        self.copies[0].start()
        self.copies[1].start()

    def got(self, *ns):
        for n in ns:
            self.copies[n].wait_recv()

    def turn(self):
        self.got(0, 1)
        self.copies[2].start()

    def end(self):
        for c in self.copies:
            c.wait_send()


class Scatter:
    def __init__(self, links, term, back, sums, via_x, via_y, from_x, from_y, send, recv, free):
        h = term.shape[0] // 2
        lo, hi = pl.ds(0, h), pl.ds(h, h)
        k = links
        self.links, self.free, self.h = k, free, h
        self.sums, self.via_x, self.via_y = sums, via_x, via_y
        self.pair = _remote(term, back, send.at[0], recv.at[0], k.c)
        routes = [(sums.at[1, lo], from_x.at[lo], k.x), (sums.at[2, hi], from_y.at[hi], k.y), (sums.at[3, lo], via_x, k.x),
                  (sums.at[3, hi], via_y, k.y), (sums.at[1, hi], from_x.at[hi], k.x), (sums.at[2, lo], from_y.at[lo], k.y)]
        self.copies = [_remote(src, dst, send.at[n + 1], recv.at[n + 1], to) for n, (src, dst, to) in enumerate(routes)]

    def room(self, j):
        @pl.when(j > 0)
        def _():
            self.pair.wait_send()

    def give(self, j):
        @pl.when(j > 0)
        def _():
            pl.semaphore_wait(self.free, 1)

        self.pair.start()

    def take(self):
        self.pair.wait_recv()

    def taken(self, j):
        @pl.when(j < 3)
        def _():
            pl.semaphore_signal(self.free, inc=1, device_id={"tp": self.links.c}, device_id_type=pl.DeviceIdType.MESH)

    def pass_on(self, pi):
        for n, at in ((0, 1), (1, 2), (2, 3), (3, 3)):

            @pl.when(pi == at)
            def _(n=n):
                self.copies[n].start()

    def finish(self):
        for n, via, pair, start in ((2, self.via_x, 2, 0), (3, self.via_y, 1, self.h)):
            self.copies[n].wait_recv()

            @_rows(self.h, ROWS)
            def _(here):
                at = _at(start + here.start, ROWS)
                self.sums[pair, at, :] = (self.sums[pair, at, :].astype(F32) + via[here, :].astype(F32)).astype(BF)

            self.copies[5 if pair == 2 else 4].start()

    def end(self, pair=True):
        if pair:
            self.pair.wait_send()
        for n in (0, 1, 4, 5):
            self.copies[n].wait_recv()
        for c in self.copies:
            c.wait_send()


def _scale_of(wide):
    return lax.rsqrt(jnp.mean(wide * wide, -1, keepdims=True) + 1e-6)


def _finish_body(x_ref, base_ref, c0_ref, fx_ref, fy_ref, *rest):
    given, (out_ref, *outs) = rest[: len(rest) // 2], rest[len(rest) // 2 :]
    for src, dst in zip(given, outs):
        dst[...] = src[...]
    g = c0_ref[...].astype(F32) + fx_ref[...].astype(F32) + fy_ref[...].astype(F32)
    wide = x_ref[...].astype(F32)
    scale = _scale_of(wide)
    along = jnp.mean(g * wide, -1, keepdims=True)
    out_ref[...] = (base_ref[...].astype(F32) + scale * (g - wide * (scale * scale * along))).astype(BF)


def finish(x, base, sums, given):
    arrays = [x, base, *sums, *given]
    specs = [pl.BlockSpec((a.shape[0] // TP, a.shape[1]), lambda i: (i, 0)) for a in arrays]
    outs = [specs[0], *specs[-len(given) :]]
    return pl.pallas_call(_finish_body, grid=(TP,), in_specs=specs, out_specs=outs, out_shape=[_like(a.shape) for a in (x, *given)], name="finish",
                          compiler_params=pltpu.CompilerParams(vmem_limit_bytes=VMEM))(*arrays)


def _turn(x, cos, sin):
    parts = [x[:, n : n + HEAD] for n in range(0, x.shape[1], HEAD)]
    return jnp.concatenate([p * cos + pltpu.roll(p, HEAD // 2, 1) * sin for p in parts], axis=1)


def _diagonal(size):
    return lax.broadcasted_iota(jnp.int32, (size, size), 1) >= lax.broadcasted_iota(jnp.int32, (size, size), 0)


def _attend_rows(iq, q, k, v, o, lse, top_s, mix_s, b=512):
    bq, width = q.shape
    heads, strips = width // HEAD, bq // b
    scale = HEAD**-0.5
    e = scale * LOG2E
    top_s[...] = jnp.full_like(top_s, NEG)
    mix_s[...] = jnp.zeros_like(mix_s)
    ones = jnp.ones((8, b), BF)

    def block(j, first):
        here = pl.ds(j * b, b)
        pieces = [(i, n) for i in range(heads) for n in range(first or 0, strips)]
        scores = [_dot_t(k[here, i * HEAD : (i + 1) * HEAD], q[n * b : (n + 1) * b, i * HEAD : (i + 1) * HEAD]) for i, n in pieces]
        weights, keeps = [], []
        for (i, n), s in zip(pieces, scores):
            if n == first:
                s = jnp.where(_diagonal(b), s, HIDDEN)
            at = slice(n * b, (n + 1) * b)
            old = top_s[i : i + 1, at]
            top = jnp.maximum(old, s.max(axis=0, keepdims=True))
            top_s[i : i + 1, at] = top
            weights.append(jnp.exp2((s - top) * e).astype(BF))
            keeps.append(jnp.exp2((old - top) * e))
        for (i, n), p, keep in zip(pieces, weights, keeps):
            at = slice(n * b, (n + 1) * b)
            values = jnp.concatenate([v[here, i * HEAD : (i + 1) * HEAD].T, ones], axis=0)
            mix_s[i, :, at] = mix_s[i, :, at] * keep + _dot(values, p)

    lax.fori_loop(0, iq * strips, lambda j, _: block(j, None), None)

    for n in range(strips):
        block(iq * strips + n, n)
    for i in range(heads):
        total = mix_s[i, HEAD : HEAD + 1, :]
        o[:, i * HEAD : (i + 1) * HEAD] = (mix_s[i, :HEAD, :] * (1 / total)).T.astype(BF)
        lse[i : i + 1, :] = top_s[i : i + 1, :] * scale + jnp.log(total)


def _attend_bwd_body(q_ref, k_ref, v_ref, do_ref, o_ref, lse_ref, cosq_ref, sinq_ref, cos_ref, sin_ref, dh_ref, dq_ref, dk_ref, dv_ref, dhs_ref,
                     dq_s, dk_s, dv_s, send, recv, *, scale, b):
    links = Links()
    gather = Gather(links, dh_ref, dhs_ref, send, recv, False)
    bq, width = q_ref.shape
    heads, strips = width // HEAD, bq // b
    iq = pl.program_id(0)
    e = scale * LOG2E

    @pl.when(iq == 0)
    def _():
        links.meet()
        gather.begin()
        dk_s[...] = jnp.zeros_like(dk_s)
        dv_s[...] = jnp.zeros_like(dv_s)

    dq_s[...] = jnp.zeros_like(dq_s)
    lses = [lse_ref[i : i + 1, :] * LOG2E for i in range(heads)]
    deltas = []
    for i in range(heads):
        at = slice(i * HEAD, (i + 1) * HEAD)
        deltas.append((do_ref[:, at].astype(F32) * o_ref[:, at].astype(F32)).T.sum(axis=0, keepdims=True))

    def block(j, first):
        here = pl.ds(j * b, b)
        pieces = [(i, n) for i in range(heads) for n in range(first or 0, strips)]
        qs = [q_ref[n * b : (n + 1) * b, i * HEAD : (i + 1) * HEAD] for i, n in pieces]
        dos = [do_ref[n * b : (n + 1) * b, i * HEAD : (i + 1) * HEAD] for i, n in pieces]
        scores = [_dot_t(k_ref[here, i * HEAD : (i + 1) * HEAD], x) for (i, _), x in zip(pieces, qs)]
        dps = [_dot_t(v_ref[here, i * HEAD : (i + 1) * HEAD], x) for (i, _), x in zip(pieces, dos)]
        for m, (i, n) in enumerate(pieces):
            at, head = slice(n * b, (n + 1) * b), slice(i * HEAD, (i + 1) * HEAD)
            p = jnp.exp2(scores[m] * e - lses[i][:, at])
            if n == first:
                p = jnp.where(_diagonal(b), p, 0.0)
            ds = (p * (dps[m] - deltas[i][:, at])).astype(BF)
            dv_s[here, head] += _dot(p.astype(BF), dos[m])
            dk_s[here, head] += _dot(ds, qs[m])
            dq_s[i, :, at] += _dot(k_ref[here, head].T, ds)

    lax.fori_loop(0, iq * strips, lambda j, _: block(j, None), None)

    @pl.when(iq == pl.num_programs(0) - 1)
    def _():
        gather.middle()

    for n in range(strips):
        block(iq * strips + n, n)

    def back(g, cos, sin):
        return _turn(g.astype(BF).astype(F32), cos, -sin).astype(BF)

    for i in range(heads):
        head = slice(i * HEAD, (i + 1) * HEAD)
        dq_ref[:, head] = back((dq_s[i] * scale).T, cosq_ref[...], sinq_ref[...])

    @pl.when(iq == pl.num_programs(0) - 1)
    def _():
        for i in range(heads):
            head = slice(i * HEAD, (i + 1) * HEAD)
            for r in range(0, dk_s.shape[0], b):
                rows = slice(r, r + b)
                dk_ref[rows, head] = back(dk_s[rows, head] * scale, cos_ref[rows, :], sin_ref[rows, :])
                dv_ref[rows, head] = dv_s[rows, head].astype(BF)
        gather.got(0, 5, 6)
        gather.end()


def attend_bwd(q, k, v, do, o, lse, cos, sin, dh, bq=1024, b=512):
    t, n = q.shape
    heads = n // HEAD
    whole = pl.BlockSpec((t, n), lambda i: (0, 0))
    rows = pl.BlockSpec((bq, n), lambda i: (i, 0))
    part = pl.BlockSpec((bq, HEAD), lambda i: (i, 0))
    table = pl.BlockSpec((t, HEAD), lambda i: (0, 0))
    return pl.pallas_call(
        functools.partial(_attend_bwd_body, scale=HEAD**-0.5, b=b), grid=(t // bq,),
        in_specs=[rows, whole, whole, rows, rows, pl.BlockSpec((heads, bq), lambda i: (0, i)), part, part, table, table, ANY],
        out_specs=[rows, whole, whole, ANY], out_shape=[_like((t, n))] * 3 + [_like((TP, *dh.shape))],
        scratch_shapes=[_vmem(heads, HEAD, bq, dtype=F32), _vmem(t, n, dtype=F32), _vmem(t, n, dtype=F32), SEMS, SEMS],
        **_talks(7, "attend_bwd", dimension_semantics=("arbitrary",)))(q, k, v, do, o, lse, cos, sin, cos, sin, dh)


def _mlp_body(own_ref, dy_ref, dys_ref, wg_hbm, wu_hbm, wd_hbm, all_ref, far_ref, hid_ref, c0_ref, from_x, from_y, bg_ref, bu_ref,
              wg, wu, wd, by_g, by_u, bv, yv, term, back, sums, via_x, via_y, hid, dg, du, load, store, wsem, gsend, grecv, fsend, frecv, ssend, srecv, free):
    k = Links()
    t, d = own_ref.shape
    f = wg.shape[1]
    n = f
    weights = [pltpu.make_async_copy(a, b, wsem.at[i]) for i, (a, b) in enumerate(((wg_hbm, wg), (wu_hbm, wu), (wd_hbm, wd)))]
    for w in weights:
        w.start()
    k.meet()
    gather = Gather(k, own_ref, all_ref, gsend, grecv)
    scatter = Scatter(k, term, back, sums, via_x, via_y, from_x, from_y, ssend, srecv, free)
    gather.begin()
    far = Far(k, dys_ref, far_ref, fsend, frecv)

    def fetch(s, par):
        y = dy_ref if s == 0 else far_ref.at[s - D] if s >= D else dys_ref.at[s]
        return [pltpu.make_async_copy(all_ref.at[s] if s else own_ref, bv.at[par], load.at[par]),
                pltpu.make_async_copy(y, yv.at[par], load.at[2 + par])]

    def start(copies):
        for c in copies:
            c.start()

    def wait(copies):
        for c in copies:
            c.wait()

    start(fetch(0, 1))
    by_g[...] = jnp.zeros_like(by_g)
    by_u[...] = jnp.zeros_like(by_u)
    gather.got(0)
    start(fetch(1, 0))
    for w in weights:
        w.wait()

    def put(s):
        return pltpu.make_async_copy(hid, hid_ref.at[s], store.at[0])

    def work(s, par, first):
        wait(fetch(1, par))

        @pl.when(jnp.logical_not(first))
        def _():
            put(0).wait()

        @_rows(f, n)
        def _(cols):
            b = bv[par]
            gate, up = _dot(b, wg[:, cols]), _dot(b, wu[:, cols])
            g = _dot_t(yv[par], wd[cols, :]).astype(BF).astype(F32)
            sig = 1 / (1 + jnp.exp(-gate))
            silu = gate * sig
            hid[:, cols] = (silu * up).astype(BF)
            du[:, cols] = (g * silu).astype(BF)
            dg[:, cols] = (g * up * (sig + silu * (1 - sig))).astype(BF)

        put(s).start()

    def weigh(par):
        @_rows(d, f)
        def _(rows):
            bt = bv[par, :, rows].T
            by_g[rows, :] += _dot(bt, dg[...])
            by_u[rows, :] += _dot(bt, du[...])

    def terms(cols):
        return _dot_t(dg[...], wg[cols, :]) + _dot_t(du[...], wu[cols, :])

    @pl.loop(0, PAIRS)
    def _(pi):
        base = 4 * lax.rem(pi, 2) + 2 * lax.div(pi, 2)
        work(base + 1, 0, pi == 0)
        scatter.room(pi)

        @_rows(d, n)
        def _(cols):
            term[:, cols] = terms(cols).astype(BF)

        scatter.give(pi)
        weigh(0)
        for at, coming, ready in ((1, YC, 6), (2, DC, 7)):

            @pl.when(pi == at)
            def _(coming=coming, ready=ready):
                gather.got(ready)
                if coming == DC:
                    far.got(2)
                start(fetch(coming, 0))

        work(base, 1, pi < 0)
        scatter.take()

        @_rows(d, n)
        def _(cols):
            sums[pi, :, cols] = (terms(cols) + back[:, cols].astype(F32)).astype(BF)

        scatter.taken(pi)
        scatter.pass_on(pi)
        weigh(1)

        @pl.when(pi == 0)
        def _():
            gather.middle()
            far.begin()
            start(fetch(X, 1))
            gather.got(5)
            start(fetch(XC, 0))

        @pl.when(pi == 1)
        def _():
            start(fetch(Y, 1))
            gather.far()
            far.turn()

        @pl.when(pi == 2)
        def _():
            start(fetch(D, 1))

    put(0).wait()
    first = pltpu.make_async_copy(sums.at[0], c0_ref, store.at[1])
    first.start()
    slots = (dg, du)
    blocks = [(acc, out, r) for acc, out in ((by_g, bg_ref), (by_u, bu_ref)) for r in range(0, d, t)]

    def leave(m):
        acc, out, r = blocks[m]
        return pltpu.make_async_copy(slots[m % 2], out.at[pl.ds(r, t), :], load.at[m % 2])

    def stage(m):
        acc, out, r = blocks[m]
        if m >= 2:
            leave(m - 2).wait()

        @_rows(t, ROWS)
        def _(here):
            slots[m % 2][here, :] = acc[_at(r + here.start, ROWS), :].astype(BF)

        leave(m).start()

    for m in range(len(blocks)):
        stage(m)
        if m == len(blocks) // 2:
            scatter.finish()
    for m in range(len(blocks) - 2, len(blocks)):
        leave(m).wait()
    first.wait()
    gather.end()
    far.end()
    scatter.end()


def mlp(b, dy, dys, wg, wu, wd):
    t, d = b.shape
    f = wg.shape[1]
    all_, far, hid, c0, fx, fy, bg, bu = pl.pallas_call(
        _mlp_body, in_specs=[ANY] * 6, out_specs=[ANY] * 8,
        out_shape=[_like((TP, t, d)), _like((2, t, d)), _like((TP, t, f))] + [_like((t, d))] * 3 + [_like((d, f))] * 2,
        scratch_shapes=[*[_vmem(d, f)] * 2, _vmem(f, d), *[_vmem(d, f, dtype=F32)] * 2, *[_vmem(2, t, d)] * 2, *[_vmem(t, d)] * 2, _vmem(PAIRS, t, d),
                        *[_vmem(t // 2, d)] * 2, *[_vmem(t, f)] * 3, *[SEMS] * 9, pltpu.SemaphoreType.REGULAR],
        **_talks(1, "mlp"))(b, dy, dys, wg, wu, wd)
    return hid, far, [c0, fx, fy], bg, bu


def _head_body(x_ref, dy_ref, wq_ref, wk_ref, wv_ref, wo_ref, base_ref, fine_ref,
               all_ref, dys_ref, q_ref, k_ref, v_ref, cos_ref, sin_ref, o_ref, lse_ref, wos_ref, h_ref, b_ref,
               w, xv, av, q, k, v, cos, sin, o, lse, top_s, mix_s, os, ws, acc, load, store, wsem, osem, asend, arecv, ysend, yrecv, wsend, wrecv, hsend, hrecv):
    links = Links()
    t, d = x_ref.shape
    n = wq_ref.shape[1]
    get = pltpu.make_async_copy(x_ref, xv, load.at[0])
    get.start()
    wl = [pltpu.make_async_copy(r, w.at[:, pl.ds(i * n, n)], wsem.at[i]) for i, r in enumerate((wq_ref, wk_ref, wv_ref))]
    for c in wl:
        c.start()
    get.wait()

    @_rows(t, ROWS)
    def _(at):
        wide = xv[at, :].astype(F32)
        av[0, at, :] = (wide * _scale_of(wide)).astype(BF)

    own = pltpu.make_async_copy(av.at[0], all_ref.at[0], store.at[0])
    own.start()
    links.meet_all()
    own.wait()
    a = Gather(links, all_ref.at[0], all_ref, asend, arecv)
    y = Gather(links, dy_ref, dys_ref, ysend, yrecv, False)
    g = Gather(links, wo_ref, wos_ref, wsend, wrecv)
    a.begin()

    def fetch(s, par):
        return pltpu.make_async_copy(all_ref.at[s], av.at[par], load.at[par])

    def work(s, par):
        fetch(s, par).wait()
        place = links.owner(s)
        bc, bs = base_ref[0, pl.ds(place, 1), :], base_ref[1, pl.ds(place, 1), :]
        sign = jnp.where(lax.broadcasted_iota(jnp.int32, (1, HEAD), 1) < HEAD // 2, -1.0, 1.0)
        got = _dot(av[par], w[...]).astype(BF)
        here = _at(place * t, t)
        fc, fs = fine_ref[0], fine_ref[1]
        c, sn = bc * fc - bs * fs, sign * (bs * fc + bc * fs)
        cos[here, :] = c
        sin[here, :] = sn
        q[here, :] = _turn(got[:, :n].astype(F32), c, sn).astype(BF)
        k[here, :] = _turn(got[:, n : 2 * n].astype(F32), c, sn).astype(BF)
        v[here, :] = got[:, 2 * n :]

    for c in wl:
        c.wait()
    fetch(0, 0).start()

    @pl.loop(0, 4)
    def _(j):
        @pl.when(j == 0)
        def _():
            a.got(0)
            fetch(1, 1).start()

        @pl.when(j == 1)
        def _():
            a.middle()
            g.begin()
            fetch(X, 0).start()
            fetch(Y, 1).start()

        @pl.when(j == 2)
        def _():
            a.got(5, 6)
            fetch(XC, 0).start()
            fetch(YC, 1).start()

        @pl.when(j == 3)
        def _():
            a.far()
            fetch(D, 0).start()
            a.got(7)
            fetch(DC, 1).start()

        work(j + 3 * lax.div(j + 3, 4), 0)
        work(j + 1 + 3 * lax.div(j, 3), 1)

    outs = [pltpu.make_async_copy(src, dst, store.at[i])
            for i, (src, dst) in enumerate(((q, q_ref), (k, k_ref), (v, v_ref), (cos, cos_ref), (sin, sin_ref), (lse, lse_ref)))]
    for c in outs[:-1]:
        c.start()
    rows = lambda s: _at(links.owner(s) * t, t)
    copies = {s: _remote(o_ref.at[rows(s), :], os.at[s], hsend.at[s], hrecv.at[s], links.owner(s)) for s in BY_DISTANCE}
    bq = q.shape[0] // 2

    @pl.loop(0, 2)
    def _(iq):
        block = _at(iq * bq, bq)
        _attend_rows(iq, q.at[block, :], k, v, o.at[block, :], lse.at[:, block], top_s, mix_s)
        put = pltpu.make_async_copy(o.at[block, :], o_ref.at[block, :], load.at[0])
        put.start()
        put.wait()
        for s in BY_DISTANCE:

            @pl.when(lax.div(links.owner(s) * t, bq) == iq)
            def _(s=s):
                copies[s].start()

        @pl.when(iq == 0)
        def _():
            g.middle()

    y.begin()
    outs[-1].start()
    mine = pltpu.make_async_copy(o_ref.at[rows(0), :], os.at[0], load.at[0])
    mine.start()
    g.far()
    g.got(0, 5, 6, 7)
    wl = [pltpu.make_async_copy(wos_ref.at[s] if s else wo_ref, ws.at[s], osem.at[s]) for s in range(TP)]
    for c in wl:
        c.start()
    mine.wait()
    for s in (ME, *BY_DISTANCE[::-1]):
        wl[s].wait()
        if s:
            copies[s].wait_recv()
        got = _dot(os[s], ws[s])
        acc[...] = acc[...] + got if s else got
    for r in range(0, t, HEAD):

        @_rows(HEAD, ROWS, r)
        def _(at):
            h = (xv[at, :].astype(F32) + acc[at, :].astype(BF).astype(F32)).astype(BF)
            xv[at, :] = h
            wide = h.astype(F32)
            av[0, at, :] = (wide * _scale_of(wide)).astype(BF)

        here = pl.ds(r, HEAD)
        for src, dst in ((xv, h_ref), (av.at[0], b_ref)):
            outs.append(pltpu.make_async_copy(src.at[here, :], dst.at[here, :], (wsem if src is xv else osem).at[r // HEAD]))
            outs[-1].start()
    for c in outs:
        c.wait()
    for c in copies.values():
        c.wait_send()
    y.middle()
    y.got(0, 5, 6)
    for c in (a, g, y):
        c.end()


def head(x, dy, wq, wk, wv, wo, base, fine):
    t, d = x.shape
    n = wq.shape[1]
    total, heads = TP * t, n // HEAD
    whole = pl.BlockSpec(memory_space=pltpu.VMEM)
    return pl.pallas_call(
        _head_body, in_specs=[*[ANY] * 6, whole, whole], out_specs=[ANY] * 12,
        out_shape=[*[_like((TP, t, d))] * 2, *[_like((total, n))] * 3, *[_like((total, HEAD), F32)] * 2, _like((total, n)), _like((heads, total), F32),
                   _like((TP, n, d)), *[_like((t, d))] * 2],
        scratch_shapes=[_vmem(d, 3 * n), _vmem(t, d), _vmem(2, t, d), *[_vmem(total, n)] * 3, *[_vmem(total, HEAD, dtype=F32)] * 2, _vmem(total, n),
                        _vmem(heads, total, dtype=F32), _vmem(heads, total // 2, dtype=F32), _vmem(heads, HEAD + 8, total // 2, dtype=F32),
                        _vmem(TP, t, n), _vmem(TP, n, d), _vmem(t, d, dtype=F32), *[SEMS] * 12],
        **_talks(2, "head"))(x, dy, wq, wk, wv, wo, base, fine)


def _part_body(h_ref, dy_ref, c0_ref, fx_ref, fy_ref, wo_ref, wos_ref, dh_ref, do_ref, ws, ins, dh, back, load, wsem, send, recv):
    k = Links()
    t, d = h_ref.shape
    q = 128
    parts = [[pltpu.make_async_copy(r.at[pl.ds(i, q), :], ins.at[m, pl.ds(i, q), :], load.at[m, i // q])
              for m, r in enumerate((h_ref, dy_ref, c0_ref, fx_ref, fy_ref))] for i in range(0, t, q)]
    for p in parts:
        for c in p:
            c.start()
    order = (*BY_DISTANCE, ME)
    wl = {s: pltpu.make_async_copy(wo_ref if s == 0 else wos_ref.at[s], ws.at[s], wsem.at[s]) for s in order}
    for s in order:
        wl[s].start()
    k.meet_all()
    out = []
    for i, p in enumerate(parts):
        for c in p:
            c.wait()

        @_rows(q, 32, i * q)
        def _(at):
            h, base, g, fx, fy = (ins[m, at, :].astype(F32) for m in range(5))
            g = g + fx + fy
            scale = _scale_of(h)
            along = jnp.mean(g * h, -1, keepdims=True)
            dh[at, :] = (base + scale * (g - h * (scale * scale * along))).astype(BF)

        here = pl.ds(i * q, q)
        out.append(pltpu.make_async_copy(dh.at[here, :], dh_ref.at[here, :], load.at[0, i]))
        out[-1].start()
    mine = _at(k.me * t, t)
    copies = {s: _remote(back.at[s], do_ref.at[mine, :], send.at[s], recv.at[s], k.owner(s)) for s in range(1, TP)}
    own = pltpu.make_async_copy(back.at[0], do_ref.at[mine, :], load.at[1, 0])
    for s in order:
        wl[s].wait()
        back[s] = _dot_t(dh[...], ws[s]).astype(BF)
        (copies[s] if s else own).start()
    for c in out:
        c.wait()
    own.wait()
    for c in copies.values():
        c.wait()


def part(h, dy, db, wo, wos):
    t, d = h.shape
    n = wo.shape[0]
    return pl.pallas_call(
        _part_body, in_specs=[ANY] * 7, out_specs=[ANY] * 2, out_shape=[_like((t, d)), _like((TP * t, n))],
        scratch_shapes=[_vmem(TP, n, d), _vmem(5, t, d), _vmem(t, d), _vmem(TP, t, n), pltpu.SemaphoreType.DMA((5, PAIRS)), *[SEMS] * 3],
        **_talks(4, "part"))(h, dy, *db, wo, wos)


def _rear_body(dq_ref, dk_ref, dv_ref, wq_ref, wk_ref, wv_ref, all_ref, o_ref, dh_ref, dhs_ref, hid_ref, dy_ref, dys_ref, far_ref,
               c0_ref, from_x, from_y, bq_ref, bk_ref, bv_ref, bo_ref, bd_ref, end_ref,
               g, w, o, av, hv, iv, yv, by_w, by_o, by_d, term, back, sums, via_x, via_y, load, gsem, wsem, ssend, srecv, esend, erecv, free):
    k = Links()
    n = dq_ref.shape[1]
    _, t, d = all_ref.shape
    f = iv.shape[2]
    gets = [pltpu.make_async_copy(r, g.at[:, pl.ds(i * n, n)], gsem.at[i]) for i, r in enumerate((dq_ref, dk_ref, dv_ref))]
    gets += [pltpu.make_async_copy(r, w.at[:, pl.ds(i * n, n)], wsem.at[i]) for i, r in enumerate((wq_ref, wk_ref, wv_ref))]
    gets.append(pltpu.make_async_copy(o_ref, o, gsem.at[3]))
    for c in gets:
        c.start()
    k.meet()
    scatter = Scatter(k, term, back, sums, via_x, via_y, from_x, from_y, ssend, srecv, free)

    last = Far(k, dhs_ref, end_ref, esend, erecv)
    last.begin()

    def fetch(s, par, h, y):
        return [pltpu.make_async_copy(src, dst.at[par], load.at[m, par])
                for m, (src, dst) in enumerate(((all_ref.at[s], av), (hid_ref.at[s], iv), (h, hv), (y, yv)))]

    def start(s, par):
        @pl.when(s == 0)
        def _():
            for c in fetch(s, par, dh_ref, dy_ref):
                c.start()

        @pl.when(jnp.logical_and(s > 0, s < D))
        def _():
            for c in fetch(s, par, dhs_ref.at[s], dys_ref.at[s]):
                c.start()

        @pl.when(s == D)
        def _():
            last.turn()

        @pl.when(s == DC)
        def _():
            last.got(2)

        @pl.when(s >= D)
        def _():
            for c in fetch(s, par, end_ref.at[lax.rem(s, 2)], far_ref.at[lax.rem(s, 2)]):
                c.start()

    start(0, 0)
    for c in gets:
        c.wait()

    def terms(s, cols):
        return _dot_t(g[_at(k.owner(s) * t, t), :], w[cols, :])

    @pl.loop(0, PAIRS)
    def _(j):
        pi = j + 3 * lax.div(3 - j, 3) - 3 * lax.div(j, 3)
        base = 4 * lax.rem(pi, 2) + 2 * lax.div(pi, 2)
        scatter.room(j)

        @_rows(d, f)
        def _(cols):
            term[:, cols] = terms(base + 1, cols).astype(BF)

        scatter.give(j)
        scatter.take()

        @_rows(d, f)
        def _(cols):
            sums[pi, :, cols] = (terms(base, cols) + back[:, cols].astype(F32)).astype(BF)

        scatter.taken(j)
        scatter.pass_on(pi)

    first = pltpu.make_async_copy(sums.at[0], c0_ref, gsem.at[0])
    first.start()

    for acc in (by_w, by_d, by_o):
        acc[...] = jnp.zeros_like(acc)

    @pl.loop(0, TP)
    def _(s):
        par = lax.rem(s, 2)
        for c in fetch(s, par, dh_ref, dy_ref):
            c.wait()

        @pl.when(s < TP - 1)
        def _():
            start(s + 1, 1 - par)

        here = _at(k.owner(s) * t, t)

        @_rows(d, f)
        def _(rows):
            by_w[rows, :] += _dot(av[par, :, rows].T, g[here, :])

        it = iv[par].T

        @_rows(d, t)
        def _(cols):
            by_d[:, cols] += _dot(it, yv[par, :, cols])

        by_o[...] += _dot(o[here, :].T, hv[par])

        @pl.when(s == 0)
        def _():
            scatter.finish()

    scatter.pair.wait_send()
    outs = []

    def leave(src, dst, sem):
        outs.append(pltpu.make_async_copy(src, dst, sem))
        outs[-1].start()

    @_rows(d, 256)
    def _(rows):
        w[rows, :] = by_w[rows, :].astype(BF)

    for i, r in enumerate((bq_ref, bk_ref, bv_ref)):
        leave(w.at[:, pl.ds(i * n, n)], r, wsem.at[i])
    for i in range(f // t):

        @_rows(t, ROWS)
        def _(rows, i=i):
            av[i, rows, :] = by_d[_at(i * t + rows.start, ROWS), :].astype(BF)

        leave(av.at[i], bd_ref.at[pl.ds(i * t, t), :], load.at[0, i])

    @_rows(n, ROWS)
    def _(rows):
        term[rows, :] = by_o[rows, :].astype(BF)

    leave(term.at[pl.ds(0, n), :], bo_ref, gsem.at[1])
    for c in [*outs, first]:
        c.wait()
    last.end()
    scatter.end(False)


def rear(gs, ws, every, o, dh, dhs, hids, dy, dys, far):
    _, t, d = every.shape
    n, f = ws[0].shape[1], hids.shape[2]
    *terms, bq, bk, bv, bo, bd, _ = pl.pallas_call(
        _rear_body, in_specs=[ANY] * 14, out_specs=[ANY] * 9,
        out_shape=[_like((t, d))] * 3 + [_like((d, n))] * 3 + [_like((n, d)), _like((f, d)), _like((2, t, d))],
        scratch_shapes=[_vmem(TP * t, 3 * n), _vmem(d, 3 * n), _vmem(TP * t, n), *[_vmem(2, t, d)] * 2, _vmem(2, t, f), _vmem(2, t, d),
                        _vmem(d, 3 * n, dtype=F32), _vmem(n, d, dtype=F32), _vmem(f, d, dtype=F32), *[_vmem(t, d)] * 2, _vmem(PAIRS, t, d),
                        *[_vmem(t // 2, d)] * 2, pltpu.SemaphoreType.DMA((PAIRS, 2)), *[SEMS] * 6, pltpu.SemaphoreType.REGULAR],
        **_talks(5, "rear"))(*gs, *ws, every, o, dh, dhs, hids, dy, dys, far)
    return terms, bq, bk, bv, bo, bd


def tables(t):
    half = HEAD // 2

    def of(places):
        angle = places.astype(F32)[:, None] * THETA ** (-jnp.arange(half, dtype=F32) / half)
        return jnp.tile(jnp.stack([jnp.cos(angle), jnp.sin(angle)]), 2)

    return of(jnp.arange(TP) * t), of(jnp.arange(t))


def layer(x, dy, wq, wk, wv, wo, wg, wu, wd):
    every, dys, q, k, v, cos, sin, o, lse, wos, h, b = head(x, dy, wq, wk, wv, wo, *tables(x.shape[0]))
    hids, far, db, by_gate, by_up = mlp(b, dy, dys, wg, wu, wd)
    dh, do = part(h, dy, db, wo, wos)
    dq, dk, dv, dhs = attend_bwd(q, k, v, do, o, lse, cos, sin, dh)
    da, *given = rear((dq, dk, dv), (wq, wk, wv), every, o, dh, dhs, hids, dy, dys, far)
    return finish(x, dh, da, (*given[:-1], by_gate, by_up, given[-1]))


def solution(mesh):
    def step(x, dy, *weights):
        dx, *rest = layer(x[0], dy[0], *weights)
        return (dx[None], *rest)

    states, by_columns, by_rows = P("dp", "tp", None), P(None, "tp"), P("tp", None)
    weights = (by_columns, by_columns, by_columns, by_rows, by_columns, by_columns, by_rows)
    own = tuple(P("dp", "tp") if spec == by_columns else P(("dp", "tp"), None) for spec in weights)
    return jax.shard_map(step, mesh=mesh, in_specs=(states, states, *weights), out_specs=(states, *own), check_vma=False)
```

```python
import functools

import jax
import jax.numpy as jnp
from jax import lax
from jax.experimental import pallas as pl
from jax.experimental.pallas import tpu as pltpu
from jax.sharding import PartitionSpec as P


HEAD = 128
THETA = 10000
NEG = -1e30
HIDDEN = 2 * NEG
LOG2E = 1.4426950408889634
VMEM = 66 * 10**6
BF = jnp.bfloat16
F32 = jnp.float32
TP = 8
PAIRS = 4
ME, C, Y, YC, X, XC, D, DC = range(TP)
BY_DISTANCE = (DC, D, XC, YC, X, Y, C)
ROWS = 64


def _dot(a, b, ca=1, cb=0):
    return lax.dot_general(a, b, (((ca,), (cb,)), ((), ())), preferred_element_type=F32)


def _dot_t(a, b):
    return _dot(a, b, 1, 1)


def _at(start, size):
    return pl.ds(pl.multiple_of(start, size), size)


def _rows(n, size, start=0):
    return lambda body: pl.loop(0, n // size)(lambda i: body(_at(start + i * size, size)))


def _talks(number, name, **more):
    params = pltpu.CompilerParams(vmem_limit_bytes=VMEM, collective_id=number, has_side_effects=True, **more)
    return {"compiler_params": params, "name": name}


ANY = pl.BlockSpec(memory_space=pl.ANY)
SEMS = pltpu.SemaphoreType.DMA((TP,))


def _vmem(*shape, dtype=BF):
    return pltpu.VMEM(shape, dtype)


def _like(shape, dtype=BF):
    return jax.ShapeDtypeStruct(shape, dtype)


class Links:
    def __init__(self):
        self.me = lax.axis_index("tp")
        self.steps = {n: n - 2 * n * lax.rem(lax.div(self.me, n), 2) for n in (C, Y, X)}
        self.c, self.y, self.x = (self.me + step for step in self.steps.values())

    def owner(self, s):
        place = self.me
        for n, step in self.steps.items():
            place = place + (step * (s // n % 2) if isinstance(s, int) else step * lax.rem(lax.div(s, n), 2))
        return place

    def meet(self):
        barrier = pltpu.get_barrier_semaphore()
        for d in (self.c, self.y, self.x):
            pl.semaphore_signal(barrier, inc=1, device_id={"tp": d}, device_id_type=pl.DeviceIdType.MESH)
        pl.semaphore_wait(barrier, 3)

    def meet_all(self):
        barrier = pltpu.get_barrier_semaphore()
        for s in range(1, TP):
            pl.semaphore_signal(barrier, inc=1, device_id={"tp": self.owner(s)}, device_id_type=pl.DeviceIdType.MESH)
        pl.semaphore_wait(barrier, TP - 1)


def _remote(src, dst, send, recv, to):
    return pltpu.make_async_remote_copy(src_ref=src, dst_ref=dst, send_sem=send, recv_sem=recv, device_id={"tp": to},
                                        device_id_type=pl.DeviceIdType.MESH)


class Gather:
    def __init__(self, links, own, every, send, recv, far=True):
        h = own.shape[0] // 2
        lo, hi = pl.ds(0, h), pl.ds(h, h)
        k = links
        routes = [(own, every.at[C], k.c), (own, every.at[X], k.x), (own, every.at[Y], k.y), (every.at[X, lo], every.at[D, lo], k.y),
                  (every.at[Y, hi], every.at[D, hi], k.x), (every.at[X], every.at[XC], k.c), (every.at[Y], every.at[YC], k.c),
                  (every.at[D], every.at[DC], k.c)]
        self.copies = {n: _remote(src, dst, send.at[n], recv.at[n], to) for n, (src, dst, to) in enumerate(routes) if far or n not in (3, 4, 7)}

    def begin(self):
        for n in (1, 2, 0):
            self.copies[n].start()

    def got(self, *ns):
        for n in ns:
            self.copies[n].wait_recv()

    def middle(self):
        self.got(1, 2)
        for n in (3, 4, 5, 6):
            if n in self.copies:
                self.copies[n].start()

    def far(self):
        self.got(3, 4)
        self.copies[7].start()

    def end(self):
        for c in self.copies.values():
            c.wait_send()


class Far:
    def __init__(self, links, every, far, send, recv, start=0):
        size, half = far.shape[1] // 2, every.shape[1] // 2
        a, b = pl.ds(0, size), pl.ds(size, size)
        self.copies = [_remote(every.at[X, pl.ds(start, size)], far.at[0, a], send.at[0], recv.at[0], links.y),
                       _remote(every.at[Y, pl.ds(half + start, size)], far.at[0, b], send.at[1], recv.at[1], links.x),
                       _remote(far.at[0], far.at[1], send.at[2], recv.at[2], links.c)]

    def begin(self):
        self.copies[0].start()
        self.copies[1].start()

    def got(self, *ns):
        for n in ns:
            self.copies[n].wait_recv()

    def turn(self):
        self.got(0, 1)
        self.copies[2].start()

    def end(self):
        for c in self.copies:
            c.wait_send()


class Scatter:
    def __init__(self, links, term, back, sums, via_x, via_y, from_x, from_y, send, recv, free):
        h = term.shape[0] // 2
        lo, hi = pl.ds(0, h), pl.ds(h, h)
        k = links
        self.links, self.free, self.h = k, free, h
        self.sums, self.via_x, self.via_y = sums, via_x, via_y
        self.pair = _remote(term, back, send.at[0], recv.at[0], k.c)
        routes = [(sums.at[1, lo], from_x.at[lo], k.x), (sums.at[2, hi], from_y.at[hi], k.y), (sums.at[3, lo], via_x, k.x),
                  (sums.at[3, hi], via_y, k.y), (sums.at[1, hi], from_x.at[hi], k.x), (sums.at[2, lo], from_y.at[lo], k.y)]
        self.copies = [_remote(src, dst, send.at[n + 1], recv.at[n + 1], to) for n, (src, dst, to) in enumerate(routes)]

    def room(self, j):
        @pl.when(j > 0)
        def _():
            self.pair.wait_send()

    def give(self, j):
        @pl.when(j > 0)
        def _():
            pl.semaphore_wait(self.free, 1)

        self.pair.start()

    def take(self):
        self.pair.wait_recv()

    def taken(self, j):
        @pl.when(j < 3)
        def _():
            pl.semaphore_signal(self.free, inc=1, device_id={"tp": self.links.c}, device_id_type=pl.DeviceIdType.MESH)

    def pass_on(self, pi):
        for n, at in ((0, 1), (1, 2), (2, 3), (3, 3)):

            @pl.when(pi == at)
            def _(n=n):
                self.copies[n].start()

    def finish(self):
        for n, via, pair, start in ((2, self.via_x, 2, 0), (3, self.via_y, 1, self.h)):
            self.copies[n].wait_recv()

            @_rows(self.h, ROWS)
            def _(here):
                at = _at(start + here.start, ROWS)
                self.sums[pair, at, :] = (self.sums[pair, at, :].astype(F32) + via[here, :].astype(F32)).astype(BF)

            self.copies[5 if pair == 2 else 4].start()

    def end(self, pair=True):
        if pair:
            self.pair.wait_send()
        for n in (0, 1, 4, 5):
            self.copies[n].wait_recv()
        for c in self.copies:
            c.wait_send()


def _scale_of(wide):
    return lax.rsqrt(jnp.mean(wide * wide, -1, keepdims=True) + 1e-6)


def _finish_body(x_ref, base_ref, c0_ref, fx_ref, fy_ref, *rest):
    given, (out_ref, *outs) = rest[: len(rest) // 2], rest[len(rest) // 2 :]
    for src, dst in zip(given, outs):
        dst[...] = src[...]
    g = c0_ref[...].astype(F32) + fx_ref[...].astype(F32) + fy_ref[...].astype(F32)
    wide = x_ref[...].astype(F32)
    scale = _scale_of(wide)
    along = jnp.mean(g * wide, -1, keepdims=True)
    out_ref[...] = (base_ref[...].astype(F32) + scale * (g - wide * (scale * scale * along))).astype(BF)


def finish(x, base, sums, given):
    arrays = [x, base, *sums, *given]
    specs = [pl.BlockSpec((a.shape[0] // TP, a.shape[1]), lambda i: (i, 0)) for a in arrays]
    outs = [specs[0], *specs[-len(given) :]]
    return pl.pallas_call(_finish_body, grid=(TP,), in_specs=specs, out_specs=outs, out_shape=[_like(a.shape) for a in (x, *given)], name="finish",
                          compiler_params=pltpu.CompilerParams(vmem_limit_bytes=VMEM))(*arrays)


def _turn(x, cos, sin):
    parts = [x[:, n : n + HEAD] for n in range(0, x.shape[1], HEAD)]
    return jnp.concatenate([p * cos + pltpu.roll(p, HEAD // 2, 1) * sin for p in parts], axis=1)


def _diagonal(size):
    return lax.broadcasted_iota(jnp.int32, (size, size), 1) >= lax.broadcasted_iota(jnp.int32, (size, size), 0)


def _attend_rows(iq, q, k, v, o, lse, top_s, mix_s, b=512):
    bq, width = q.shape
    heads, strips = width // HEAD, bq // b
    scale = HEAD**-0.5
    e = scale * LOG2E
    top_s[...] = jnp.full_like(top_s, NEG)
    mix_s[...] = jnp.zeros_like(mix_s)
    ones = jnp.ones((8, b), BF)

    def block(j, first):
        here = pl.ds(j * b, b)
        pieces = [(i, n) for i in range(heads) for n in range(first or 0, strips)]
        scores = [_dot_t(k[here, i * HEAD : (i + 1) * HEAD], q[n * b : (n + 1) * b, i * HEAD : (i + 1) * HEAD]) for i, n in pieces]
        weights, keeps = [], []
        for (i, n), s in zip(pieces, scores):
            if n == first:
                s = jnp.where(_diagonal(b), s, HIDDEN)
            at = slice(n * b, (n + 1) * b)
            old = top_s[i : i + 1, at]
            top = jnp.maximum(old, s.max(axis=0, keepdims=True))
            top_s[i : i + 1, at] = top
            weights.append(jnp.exp2((s - top) * e).astype(BF))
            keeps.append(jnp.exp2((old - top) * e))
        for (i, n), p, keep in zip(pieces, weights, keeps):
            at = slice(n * b, (n + 1) * b)
            values = jnp.concatenate([v[here, i * HEAD : (i + 1) * HEAD].T, ones], axis=0)
            mix_s[i, :, at] = mix_s[i, :, at] * keep + _dot(values, p)

    lax.fori_loop(0, iq * strips, lambda j, _: block(j, None), None)

    for n in range(strips):
        block(iq * strips + n, n)
    for i in range(heads):
        total = mix_s[i, HEAD : HEAD + 1, :]
        o[:, i * HEAD : (i + 1) * HEAD] = (mix_s[i, :HEAD, :] * (1 / total)).T.astype(BF)
        lse[i : i + 1, :] = top_s[i : i + 1, :] * scale + jnp.log(total)


def _attend_bwd_body(q_ref, k_ref, v_ref, do_ref, o_ref, lse_ref, cosq_ref, sinq_ref, cos_ref, sin_ref, dh_ref, dq_ref, dk_ref, dv_ref, dhs_ref, early_ref,
                     dq_s, dk_s, dv_s, send, recv, esend, erecv, *, scale, b):
    links = Links()
    gather = Gather(links, dh_ref, dhs_ref, send, recv, False)
    early = Far(links, dhs_ref, early_ref, esend, erecv)
    bq, width = q_ref.shape
    heads, strips = width // HEAD, bq // b
    iq = pl.program_id(0)
    e = scale * LOG2E

    @pl.when(iq == 0)
    def _():
        links.meet()
        gather.begin()
        dk_s[...] = jnp.zeros_like(dk_s)
        dv_s[...] = jnp.zeros_like(dv_s)

    dq_s[...] = jnp.zeros_like(dq_s)
    lses = [lse_ref[i : i + 1, :] * LOG2E for i in range(heads)]
    deltas = []
    for i in range(heads):
        at = slice(i * HEAD, (i + 1) * HEAD)
        deltas.append((do_ref[:, at].astype(F32) * o_ref[:, at].astype(F32)).T.sum(axis=0, keepdims=True))

    def block(j, first):
        here = pl.ds(j * b, b)
        pieces = [(i, n) for i in range(heads) for n in range(first or 0, strips)]
        qs = [q_ref[n * b : (n + 1) * b, i * HEAD : (i + 1) * HEAD] for i, n in pieces]
        dos = [do_ref[n * b : (n + 1) * b, i * HEAD : (i + 1) * HEAD] for i, n in pieces]
        scores = [_dot_t(k_ref[here, i * HEAD : (i + 1) * HEAD], x) for (i, _), x in zip(pieces, qs)]
        dps = [_dot_t(v_ref[here, i * HEAD : (i + 1) * HEAD], x) for (i, _), x in zip(pieces, dos)]
        for m, (i, n) in enumerate(pieces):
            at, head = slice(n * b, (n + 1) * b), slice(i * HEAD, (i + 1) * HEAD)
            p = jnp.exp2(scores[m] * e - lses[i][:, at])
            if n == first:
                p = jnp.where(_diagonal(b), p, 0.0)
            ds = (p * (dps[m] - deltas[i][:, at])).astype(BF)
            dv_s[here, head] += _dot(p.astype(BF), dos[m])
            dk_s[here, head] += _dot(ds, qs[m])
            dq_s[i, :, at] += _dot(k_ref[here, head].T, ds)

    lax.fori_loop(0, iq * strips, lambda j, _: block(j, None), None)

    @pl.when(iq == pl.num_programs(0) - 1)
    def _():
        gather.middle()
        early.begin()

    for n in range(strips):
        block(iq * strips + n, n)

    def back(g, cos, sin):
        return _turn(g.astype(BF).astype(F32), cos, -sin).astype(BF)

    for i in range(heads):
        head = slice(i * HEAD, (i + 1) * HEAD)
        dq_ref[:, head] = back((dq_s[i] * scale).T, cosq_ref[...], sinq_ref[...])

    @pl.when(iq == pl.num_programs(0) - 1)
    def _():
        for i in range(heads):
            head = slice(i * HEAD, (i + 1) * HEAD)
            for r in range(0, dk_s.shape[0], b):
                rows = slice(r, r + b)
                dk_ref[rows, head] = back(dk_s[rows, head] * scale, cos_ref[rows, :], sin_ref[rows, :])
                dv_ref[rows, head] = dv_s[rows, head].astype(BF)
        early.turn()
        gather.got(0, 5, 6)
        early.got(2)
        gather.end()
        early.end()


def attend_bwd(q, k, v, do, o, lse, cos, sin, dh, bq=1024, b=512):
    t, n = q.shape
    heads = n // HEAD
    whole = pl.BlockSpec((t, n), lambda i: (0, 0))
    rows = pl.BlockSpec((bq, n), lambda i: (i, 0))
    part = pl.BlockSpec((bq, HEAD), lambda i: (i, 0))
    table = pl.BlockSpec((t, HEAD), lambda i: (0, 0))
    return pl.pallas_call(
        functools.partial(_attend_bwd_body, scale=HEAD**-0.5, b=b), grid=(t // bq,),
        in_specs=[rows, whole, whole, rows, rows, pl.BlockSpec((heads, bq), lambda i: (0, i)), part, part, table, table, ANY],
        out_specs=[rows, whole, whole, ANY, ANY],
        out_shape=[_like((t, n))] * 3 + [_like((TP, *dh.shape)), _like((2, dh.shape[0] // 2, dh.shape[1]))],
        scratch_shapes=[_vmem(heads, HEAD, bq, dtype=F32), _vmem(t, n, dtype=F32), _vmem(t, n, dtype=F32), *[SEMS] * 4],
        **_talks(7, "attend_bwd", dimension_semantics=("arbitrary",)))(q, k, v, do, o, lse, cos, sin, cos, sin, dh)


def _mlp_body(own_ref, dy_ref, dys_ref, wg_hbm, wu_hbm, wd_hbm, all_ref, far_ref, hid_ref, c0_ref, from_x, from_y, bg_ref, bu_ref,
              wg, wu, wd, by_g, by_u, bv, yv, term, back, sums, via_x, via_y, hid, dg, du, load, store, wsem, gsend, grecv, fsend, frecv, ssend, srecv, free):
    k = Links()
    t, d = own_ref.shape
    f = wg.shape[1]
    n = f
    weights = [pltpu.make_async_copy(a, b, wsem.at[i]) for i, (a, b) in enumerate(((wg_hbm, wg), (wu_hbm, wu), (wd_hbm, wd)))]
    for w in weights:
        w.start()
    k.meet()
    gather = Gather(k, own_ref, all_ref, gsend, grecv)
    scatter = Scatter(k, term, back, sums, via_x, via_y, from_x, from_y, ssend, srecv, free)
    gather.begin()
    far = Far(k, dys_ref, far_ref, fsend, frecv)

    def fetch(s, par):
        y = dy_ref if s == 0 else far_ref.at[s - D] if s >= D else dys_ref.at[s]
        return [pltpu.make_async_copy(all_ref.at[s] if s else own_ref, bv.at[par], load.at[par]),
                pltpu.make_async_copy(y, yv.at[par], load.at[2 + par])]

    def start(copies):
        for c in copies:
            c.start()

    def wait(copies):
        for c in copies:
            c.wait()

    start(fetch(0, 1))
    by_g[...] = jnp.zeros_like(by_g)
    by_u[...] = jnp.zeros_like(by_u)
    gather.got(0)
    start(fetch(1, 0))
    for w in weights:
        w.wait()

    def put(s):
        return pltpu.make_async_copy(hid, hid_ref.at[s], store.at[0])

    def work(s, par, first):
        wait(fetch(1, par))

        @pl.when(jnp.logical_not(first))
        def _():
            put(0).wait()

        @_rows(f, n)
        def _(cols):
            b = bv[par]
            gate, up = _dot(b, wg[:, cols]), _dot(b, wu[:, cols])
            g = _dot_t(yv[par], wd[cols, :]).astype(BF).astype(F32)
            sig = 1 / (1 + jnp.exp(-gate))
            silu = gate * sig
            hid[:, cols] = (silu * up).astype(BF)
            du[:, cols] = (g * silu).astype(BF)
            dg[:, cols] = (g * up * (sig + silu * (1 - sig))).astype(BF)

        put(s).start()

    def weigh(par):
        @_rows(d, f)
        def _(rows):
            bt = bv[par, :, rows].T
            by_g[rows, :] += _dot(bt, dg[...])
            by_u[rows, :] += _dot(bt, du[...])

    def terms(cols):
        return _dot_t(dg[...], wg[cols, :]) + _dot_t(du[...], wu[cols, :])

    @pl.loop(0, TP)
    def _(step):
        pi, par = lax.div(step, 2), lax.rem(step, 2)
        odd, even = par == 0, par == 1
        work(4 * lax.rem(pi, 2) + 2 * lax.div(pi, 2) + 1 - par, par, step == 0)

        @pl.when(odd)
        def _():
            scatter.room(pi)

            @_rows(d, n)
            def _(cols):
                term[:, cols] = terms(cols).astype(BF)

            scatter.give(pi)

        @pl.when(even)
        def _():
            scatter.take()

            @_rows(d, n)
            def _(cols):
                sums[pi, :, cols] = (terms(cols) + back[:, cols].astype(F32)).astype(BF)

            scatter.taken(pi)
            scatter.pass_on(pi)

        weigh(par)

        @pl.when(step == 1)
        def _():
            gather.middle()
            far.begin()
            start(fetch(X, 1))
            gather.got(5)
            start(fetch(XC, 0))

        @pl.when(step == 2)
        def _():
            gather.got(6)
            start(fetch(YC, 0))

        @pl.when(step == 3)
        def _():
            start(fetch(Y, 1))
            gather.far()
            far.turn()

        @pl.when(step == 4)
        def _():
            gather.got(7)
            far.got(2)
            start(fetch(DC, 0))

        @pl.when(step == 5)
        def _():
            start(fetch(D, 1))

    put(0).wait()
    first = pltpu.make_async_copy(sums.at[0], c0_ref, store.at[1])
    first.start()
    slots = (dg, du)
    blocks = [(acc, out, r) for acc, out in ((by_g, bg_ref), (by_u, bu_ref)) for r in range(0, d, t)]

    def leave(m):
        acc, out, r = blocks[m]
        return pltpu.make_async_copy(slots[m % 2], out.at[pl.ds(r, t), :], load.at[m % 2])

    def stage(m):
        acc, out, r = blocks[m]
        if m >= 2:
            leave(m - 2).wait()

        @_rows(t, ROWS)
        def _(here):
            slots[m % 2][here, :] = acc[_at(r + here.start, ROWS), :].astype(BF)

        leave(m).start()

    for m in range(len(blocks)):
        stage(m)
        if m == len(blocks) // 2:
            scatter.finish()
    for m in range(len(blocks) - 2, len(blocks)):
        leave(m).wait()
    first.wait()
    gather.end()
    far.end()
    scatter.end()


def mlp(b, dy, dys, wg, wu, wd):
    t, d = b.shape
    f = wg.shape[1]
    all_, far, hid, c0, fx, fy, bg, bu = pl.pallas_call(
        _mlp_body, in_specs=[ANY] * 6, out_specs=[ANY] * 8,
        out_shape=[_like((TP, t, d)), _like((2, t, d)), _like((TP, t, f))] + [_like((t, d))] * 3 + [_like((d, f))] * 2,
        scratch_shapes=[*[_vmem(d, f)] * 2, _vmem(f, d), *[_vmem(d, f, dtype=F32)] * 2, *[_vmem(2, t, d)] * 2, *[_vmem(t, d)] * 2, _vmem(PAIRS, t, d),
                        *[_vmem(t // 2, d)] * 2, *[_vmem(t, f)] * 3, *[SEMS] * 9, pltpu.SemaphoreType.REGULAR],
        **_talks(1, "mlp"))(b, dy, dys, wg, wu, wd)
    return hid, far, [c0, fx, fy], bg, bu


def _head_body(x_ref, dy_ref, wq_ref, wk_ref, wv_ref, wo_ref, base_ref, fine_ref,
               all_ref, dys_ref, q_ref, k_ref, v_ref, cos_ref, sin_ref, o_ref, lse_ref, wos_ref, h_ref, b_ref,
               w, xv, av, q, k, v, cos, sin, o, lse, top_s, mix_s, os, ws, acc, load, store, wsem, osem, asend, arecv, ysend, yrecv, wsend, wrecv, hsend, hrecv):
    links = Links()
    t, d = x_ref.shape
    n = wq_ref.shape[1]
    get = pltpu.make_async_copy(x_ref, xv, load.at[0])
    get.start()
    wl = [pltpu.make_async_copy(r, w.at[:, pl.ds(i * n, n)], wsem.at[i]) for i, r in enumerate((wq_ref, wk_ref, wv_ref))]
    for c in wl:
        c.start()
    get.wait()

    @_rows(t, ROWS)
    def _(at):
        wide = xv[at, :].astype(F32)
        av[0, at, :] = (wide * _scale_of(wide)).astype(BF)

    own = pltpu.make_async_copy(av.at[0], all_ref.at[0], store.at[0])
    own.start()
    links.meet_all()
    own.wait()
    a = Gather(links, all_ref.at[0], all_ref, asend, arecv)
    y = Gather(links, dy_ref, dys_ref, ysend, yrecv, False)
    g = Gather(links, wo_ref, wos_ref, wsend, wrecv)
    a.begin()

    def fetch(s, par):
        return pltpu.make_async_copy(all_ref.at[s], av.at[par], load.at[par])

    def work(s, par):
        fetch(s, par).wait()
        place = links.owner(s)
        bc, bs = base_ref[0, pl.ds(place, 1), :], base_ref[1, pl.ds(place, 1), :]
        sign = jnp.where(lax.broadcasted_iota(jnp.int32, (1, HEAD), 1) < HEAD // 2, -1.0, 1.0)
        got = _dot(av[par], w[...]).astype(BF)
        here = _at(place * t, t)
        fc, fs = fine_ref[0], fine_ref[1]
        c, sn = bc * fc - bs * fs, sign * (bs * fc + bc * fs)
        cos[here, :] = c
        sin[here, :] = sn
        q[here, :] = _turn(got[:, :n].astype(F32), c, sn).astype(BF)
        k[here, :] = _turn(got[:, n : 2 * n].astype(F32), c, sn).astype(BF)
        v[here, :] = got[:, 2 * n :]

    for c in wl:
        c.wait()
    fetch(0, 0).start()

    @pl.loop(0, 4)
    def _(j):
        @pl.when(j == 0)
        def _():
            a.got(0)
            fetch(1, 1).start()

        @pl.when(j == 1)
        def _():
            a.middle()
            g.begin()
            fetch(X, 0).start()
            fetch(Y, 1).start()

        @pl.when(j == 2)
        def _():
            a.got(5, 6)
            fetch(XC, 0).start()
            fetch(YC, 1).start()

        @pl.when(j == 3)
        def _():
            a.far()
            fetch(D, 0).start()
            a.got(7)
            fetch(DC, 1).start()

        work(j + 3 * lax.div(j + 3, 4), 0)
        work(j + 1 + 3 * lax.div(j, 3), 1)

    outs = [pltpu.make_async_copy(src, dst, store.at[i])
            for i, (src, dst) in enumerate(((q, q_ref), (k, k_ref), (v, v_ref), (cos, cos_ref), (sin, sin_ref), (lse, lse_ref)))]
    for c in outs[:-1]:
        c.start()
    rows = lambda s: _at(links.owner(s) * t, t)
    copies = {s: _remote(o_ref.at[rows(s), :], os.at[s], hsend.at[s], hrecv.at[s], links.owner(s)) for s in BY_DISTANCE}
    bq = q.shape[0] // 2

    @pl.loop(0, 2)
    def _(iq):
        block = _at(iq * bq, bq)
        _attend_rows(iq, q.at[block, :], k, v, o.at[block, :], lse.at[:, block], top_s, mix_s)
        put = pltpu.make_async_copy(o.at[block, :], o_ref.at[block, :], load.at[0])
        put.start()
        put.wait()
        for s in BY_DISTANCE:

            @pl.when(lax.div(links.owner(s) * t, bq) == iq)
            def _(s=s):
                copies[s].start()

        @pl.when(iq == 0)
        def _():
            g.middle()

    y.begin()
    outs[-1].start()
    mine = pltpu.make_async_copy(o_ref.at[rows(0), :], os.at[0], load.at[0])
    mine.start()
    g.far()
    g.got(0, 5, 6, 7)
    wl = [pltpu.make_async_copy(wos_ref.at[s] if s else wo_ref, ws.at[s], osem.at[s]) for s in range(TP)]
    for c in wl:
        c.start()
    mine.wait()
    for s in (ME, *BY_DISTANCE[::-1]):
        wl[s].wait()
        if s:
            copies[s].wait_recv()
        got = _dot(os[s], ws[s])
        acc[...] = acc[...] + got if s else got
    for r in range(0, t, HEAD):

        @_rows(HEAD, ROWS, r)
        def _(at):
            h = (xv[at, :].astype(F32) + acc[at, :].astype(BF).astype(F32)).astype(BF)
            xv[at, :] = h
            wide = h.astype(F32)
            av[0, at, :] = (wide * _scale_of(wide)).astype(BF)

        here = pl.ds(r, HEAD)
        for src, dst in ((xv, h_ref), (av.at[0], b_ref)):
            outs.append(pltpu.make_async_copy(src.at[here, :], dst.at[here, :], (wsem if src is xv else osem).at[r // HEAD]))
            outs[-1].start()
    for c in outs:
        c.wait()
    for c in copies.values():
        c.wait_send()
    y.middle()
    y.got(0, 5, 6)
    for c in (a, g, y):
        c.end()


def head(x, dy, wq, wk, wv, wo, base, fine):
    t, d = x.shape
    n = wq.shape[1]
    total, heads = TP * t, n // HEAD
    whole = pl.BlockSpec(memory_space=pltpu.VMEM)
    return pl.pallas_call(
        _head_body, in_specs=[*[ANY] * 6, whole, whole], out_specs=[ANY] * 12,
        out_shape=[*[_like((TP, t, d))] * 2, *[_like((total, n))] * 3, *[_like((total, HEAD), F32)] * 2, _like((total, n)), _like((heads, total), F32),
                   _like((TP, n, d)), *[_like((t, d))] * 2],
        scratch_shapes=[_vmem(d, 3 * n), _vmem(t, d), _vmem(2, t, d), *[_vmem(total, n)] * 3, *[_vmem(total, HEAD, dtype=F32)] * 2, _vmem(total, n),
                        _vmem(heads, total, dtype=F32), _vmem(heads, total // 2, dtype=F32), _vmem(heads, HEAD + 8, total // 2, dtype=F32),
                        _vmem(TP, t, n), _vmem(TP, n, d), _vmem(t, d, dtype=F32), *[SEMS] * 12],
        **_talks(2, "head"))(x, dy, wq, wk, wv, wo, base, fine)


def _part_body(h_ref, dy_ref, c0_ref, fx_ref, fy_ref, wo_ref, wos_ref, dh_ref, do_ref, ws, ins, dh, back, load, wsem, send, recv):
    k = Links()
    t, d = h_ref.shape
    q = 128
    parts = [[pltpu.make_async_copy(r.at[pl.ds(i, q), :], ins.at[m, pl.ds(i, q), :], load.at[m, i // q])
              for m, r in enumerate((h_ref, dy_ref, c0_ref, fx_ref, fy_ref))] for i in range(0, t, q)]
    for p in parts:
        for c in p:
            c.start()
    order = (*BY_DISTANCE, ME)
    wl = {s: pltpu.make_async_copy(wo_ref if s == 0 else wos_ref.at[s], ws.at[s], wsem.at[s]) for s in order}
    for s in order:
        wl[s].start()
    k.meet_all()
    out = []
    for i, p in enumerate(parts):
        for c in p:
            c.wait()

        @_rows(q, 32, i * q)
        def _(at):
            h, base, g, fx, fy = (ins[m, at, :].astype(F32) for m in range(5))
            g = g + fx + fy
            scale = _scale_of(h)
            along = jnp.mean(g * h, -1, keepdims=True)
            dh[at, :] = (base + scale * (g - h * (scale * scale * along))).astype(BF)

        here = pl.ds(i * q, q)
        out.append(pltpu.make_async_copy(dh.at[here, :], dh_ref.at[here, :], load.at[0, i]))
        out[-1].start()
    mine = _at(k.me * t, t)
    copies = {s: _remote(back.at[s], do_ref.at[mine, :], send.at[s], recv.at[s], k.owner(s)) for s in range(1, TP)}
    own = pltpu.make_async_copy(back.at[0], do_ref.at[mine, :], load.at[1, 0])
    for s in order:
        wl[s].wait()
        back[s] = _dot_t(dh[...], ws[s]).astype(BF)
        (copies[s] if s else own).start()
    for c in out:
        c.wait()
    own.wait()
    for c in copies.values():
        c.wait()


def part(h, dy, db, wo, wos):
    t, d = h.shape
    n = wo.shape[0]
    return pl.pallas_call(
        _part_body, in_specs=[ANY] * 7, out_specs=[ANY] * 2, out_shape=[_like((t, d)), _like((TP * t, n))],
        scratch_shapes=[_vmem(TP, n, d), _vmem(5, t, d), _vmem(t, d), _vmem(TP, t, n), pltpu.SemaphoreType.DMA((5, PAIRS)), *[SEMS] * 3],
        **_talks(4, "part"))(h, dy, *db, wo, wos)


def _rear_body(dq_ref, dk_ref, dv_ref, wq_ref, wk_ref, wv_ref, all_ref, o_ref, dh_ref, dhs_ref, early_ref, hid_ref, dy_ref, dys_ref, far_ref,
               c0_ref, from_x, from_y, bq_ref, bk_ref, bv_ref, bo_ref, bd_ref, end_ref,
               g, w, o, av, hv, iv, yv, by_w, by_o, by_d, term, back, sums, via_x, via_y, load, gsem, wsem, ssend, srecv, esend, erecv, free):
    k = Links()
    n = dq_ref.shape[1]
    _, t, d = all_ref.shape
    f = iv.shape[2]
    gets = [pltpu.make_async_copy(r, g.at[:, pl.ds(i * n, n)], gsem.at[i]) for i, r in enumerate((dq_ref, dk_ref, dv_ref))]
    gets += [pltpu.make_async_copy(r, w.at[:, pl.ds(i * n, n)], wsem.at[i]) for i, r in enumerate((wq_ref, wk_ref, wv_ref))]
    gets.append(pltpu.make_async_copy(o_ref, o, gsem.at[3]))
    for c in gets:
        c.start()
    k.meet()
    scatter = Scatter(k, term, back, sums, via_x, via_y, from_x, from_y, ssend, srecv, free)

    part = t // 4
    last = Far(k, dhs_ref, end_ref, esend, erecv, part)
    last.begin()

    def fetch(s, par, h, y):
        return [pltpu.make_async_copy(src, dst.at[par], load.at[m, par])
                for m, (src, dst) in enumerate(((all_ref.at[s], av), (hid_ref.at[s], iv), (h, hv), (y, yv)))]

    def start(s, par):
        @pl.when(s == 0)
        def _():
            for c in fetch(s, par, dh_ref, dy_ref):
                c.start()

        @pl.when(jnp.logical_and(s > 0, s < D))
        def _():
            for c in fetch(s, par, dhs_ref.at[s], dys_ref.at[s]):
                c.start()

        @pl.when(s == D)
        def _():
            last.turn()

        @pl.when(s == DC)
        def _():
            last.got(2)

        @pl.when(s >= D)
        def _():
            which = lax.rem(s, 2)
            for n, c in enumerate(fetch(s, par, dh_ref, far_ref.at[which])):
                if n != 2:
                    c.start()
            for i, (r, at) in enumerate(((early_ref, 0), (end_ref, 0), (early_ref, part), (end_ref, part))):
                pltpu.make_async_copy(r.at[which, pl.ds(at, part), :], hv.at[par, pl.ds(i * part, part), :], load.at[2, par]).start()

    start(0, 0)
    for c in gets:
        c.wait()

    def terms(s, cols):
        return _dot_t(g[_at(k.owner(s) * t, t), :], w[cols, :])

    for acc in (by_w, by_d, by_o):
        acc[...] = jnp.zeros_like(acc)

    def fill(s):
        par = lax.rem(s, 2)
        for c in fetch(s, par, dh_ref, dy_ref):
            c.wait()

        @pl.when(s < DC)
        def _():
            start(s + 1, 1 - par)

        here = _at(k.owner(s) * t, t)

        @_rows(d, f)
        def _(rows):
            by_w[rows, :] += _dot(av[par, :, rows].T, g[here, :])

        it = iv[par].T

        @_rows(d, t)
        def _(cols):
            by_d[:, cols] += _dot(it, yv[par, :, cols])

        by_o[...] += _dot(o[here, :].T, hv[par])

    @pl.loop(0, TP)
    def _(s):
        pi = s + 3 * lax.div(3 - s, 3) - 3 * lax.div(s, 3)
        base = 4 * lax.rem(pi, 2) + 2 * lax.div(pi, 2)

        @pl.when(s < PAIRS)
        def _():
            scatter.room(s)

            @_rows(d, f)
            def _(cols):
                term[:, cols] = terms(base + 1, cols).astype(BF)

            scatter.give(s)

        fill(s)

        @pl.when(s < PAIRS)
        def _():
            scatter.take()

            @_rows(d, f)
            def _(cols):
                sums[pi, :, cols] = (terms(base, cols) + back[:, cols].astype(F32)).astype(BF)

            scatter.taken(s)
            scatter.pass_on(pi)

        @pl.when(s == PAIRS)
        def _():
            scatter.finish()

    first = pltpu.make_async_copy(sums.at[0], c0_ref, gsem.at[0])
    first.start()
    scatter.pair.wait_send()
    outs = []

    def leave(src, dst, sem):
        outs.append(pltpu.make_async_copy(src, dst, sem))
        outs[-1].start()

    @_rows(d, 256)
    def _(rows):
        w[rows, :] = by_w[rows, :].astype(BF)

    for i, r in enumerate((bq_ref, bk_ref, bv_ref)):
        leave(w.at[:, pl.ds(i * n, n)], r, wsem.at[i])
    for i in range(f // t):

        @_rows(t, ROWS)
        def _(rows, i=i):
            av[i, rows, :] = by_d[_at(i * t + rows.start, ROWS), :].astype(BF)

        leave(av.at[i], bd_ref.at[pl.ds(i * t, t), :], load.at[0, i])

    @_rows(n, ROWS)
    def _(rows):
        term[rows, :] = by_o[rows, :].astype(BF)

    leave(term.at[pl.ds(0, n), :], bo_ref, gsem.at[1])
    for c in [*outs, first]:
        c.wait()
    last.end()
    scatter.end(False)


def rear(gs, ws, every, o, dh, dhs, early, hids, dy, dys, far):
    _, t, d = every.shape
    n, f = ws[0].shape[1], hids.shape[2]
    *terms, bq, bk, bv, bo, bd, _ = pl.pallas_call(
        _rear_body, in_specs=[ANY] * 15, out_specs=[ANY] * 9,
        out_shape=[_like((t, d))] * 3 + [_like((d, n))] * 3 + [_like((n, d)), _like((f, d)), _like((2, t // 2, d))],
        scratch_shapes=[_vmem(TP * t, 3 * n), _vmem(d, 3 * n), _vmem(TP * t, n), *[_vmem(2, t, d)] * 2, _vmem(2, t, f), _vmem(2, t, d),
                        _vmem(d, 3 * n, dtype=F32), _vmem(n, d, dtype=F32), _vmem(f, d, dtype=F32), *[_vmem(t, d)] * 2, _vmem(PAIRS, t, d),
                        *[_vmem(t // 2, d)] * 2, pltpu.SemaphoreType.DMA((PAIRS, 2)), *[SEMS] * 6, pltpu.SemaphoreType.REGULAR],
        **_talks(5, "rear"))(*gs, *ws, every, o, dh, dhs, early, hids, dy, dys, far)
    return terms, bq, bk, bv, bo, bd


def tables(t):
    half = HEAD // 2

    def of(places):
        angle = places.astype(F32)[:, None] * THETA ** (-jnp.arange(half, dtype=F32) / half)
        return jnp.tile(jnp.stack([jnp.cos(angle), jnp.sin(angle)]), 2)

    return of(jnp.arange(TP) * t), of(jnp.arange(t))


def layer(x, dy, wq, wk, wv, wo, wg, wu, wd):
    every, dys, q, k, v, cos, sin, o, lse, wos, h, b = head(x, dy, wq, wk, wv, wo, *tables(x.shape[0]))
    hids, far, db, by_gate, by_up = mlp(b, dy, dys, wg, wu, wd)
    dh, do = part(h, dy, db, wo, wos)
    dq, dk, dv, dhs, early = attend_bwd(q, k, v, do, o, lse, cos, sin, dh)
    da, *given = rear((dq, dk, dv), (wq, wk, wv), every, o, dh, dhs, early, hids, dy, dys, far)
    return finish(x, dh, da, (*given[:-1], by_gate, by_up, given[-1]))


def solution(mesh):
    def step(x, dy, *weights):
        dx, *rest = layer(x[0], dy[0], *weights)
        return (dx[None], *rest)

    states, by_columns, by_rows = P("dp", "tp", None), P(None, "tp"), P("tp", None)
    weights = (by_columns, by_columns, by_columns, by_rows, by_columns, by_columns, by_rows)
    own = tuple(P("dp", "tp") if spec == by_columns else P(("dp", "tp"), None) for spec in weights)
    return jax.shard_map(step, mesh=mesh, in_specs=(states, states, *weights), out_specs=(states, *own), check_vma=False)
```
